32 devices in a mesh: model: 4 (over z), data: 8 (over y, x, core).
Axes of the slice: x: 2, y: 2, z: 4, core: 2. Of those that a mesh axis runs over, the one named last changes fastest.
Arguments:
- grad_qkv: float32 [8, 2, 1024, 3072], P('data', None, None, 'model')
- weight_qkv: float32 [2, 1024, 3072], P(None, 'data', 'model')
- moment1_qkv: float32 [2, 1024, 3072], P(None, 'data', 'model')
- moment2_qkv: float32 [2, 1024, 3072], P(None, 'data', 'model')
- grad_proj: float32 [8, 2, 1024, 1024], P('data', None, 'model')
- weight_proj: float32 [2, 1024, 1024], P(None, ('model', 'data'))
- moment1_proj: float32 [2, 1024, 1024], P(None, ('model', 'data'))
- moment2_proj: float32 [2, 1024, 1024], P(None, ('model', 'data'))
- grad_fcin: float32 [8, 2, 1024, 4096], P('data', None, None, 'model')
- weight_fcin: float32 [2, 1024, 4096], P(None, 'data', 'model')
- moment1_fcin: float32 [2, 1024, 4096], P(None, 'data', 'model')
- moment2_fcin: float32 [2, 1024, 4096], P(None, 'data', 'model')
- grad_fcout: float32 [8, 2, 4096, 1024], P('data', None, 'model')
- weight_fcout: float32 [2, 4096, 1024], P(None, ('model', 'data'))
- moment1_fcout: float32 [2, 4096, 1024], P(None, ('model', 'data'))
- moment2_fcout: float32 [2, 4096, 1024], P(None, ('model', 'data'))
Outputs:
- output 1: bfloat16 [2, 1024, 3072], P(None, None, 'model')
- output 2: bfloat16 [2, 1024, 1024], P(None, 'model')
- output 3: bfloat16 [2, 1024, 4096], P(None, None, 'model')
- output 4: bfloat16 [2, 4096, 1024], P(None, 'model')
- output 5: float32 [2, 1024, 3072], P(None, 'data', 'model')
- output 6: float32 [2, 1024, 1024], P(None, ('model', 'data'))
- output 7: float32 [2, 1024, 4096], P(None, 'data', 'model')
- output 8: float32 [2, 4096, 1024], P(None, ('model', 'data'))
- output 9: float32 [2, 1024, 3072], P(None, 'data', 'model')
- output 10: float32 [2, 1024, 1024], P(None, ('model', 'data'))
- output 11: float32 [2, 1024, 4096], P(None, 'data', 'model')
- output 12: float32 [2, 4096, 1024], P(None, ('model', 'data'))
- output 13: float32 [2, 1024, 3072], P(None, 'data', 'model')
- output 14: float32 [2, 1024, 1024], P(None, ('model', 'data'))
- output 15: float32 [2, 1024, 4096], P(None, 'data', 'model')
- output 16: float32 [2, 4096, 1024], P(None, ('model', 'data'))
All inputs are finite; a program needn't handle non-finite values.
Results may differ from the reference program's by a relative error of at most 0.001.
Values are sent between devices in bfloat16 or wider.
A program may use at most 1 GiB of HBM per device.

```python
import jax
import jax.numpy as jnp

D_MODEL = 1024
FF_DIM = 4096
LAYERS = 2
DATA_SIZE = 8
STEP_COUNT = 100

LEARN_RATE = 0.08
BETA_ONE = 0.9
BETA_TWO = 0.999
ADAM_EPS = 1e-6
DECAY_RATE = 0.01
MAX_NORM = 1.0
TILT_RATE = 0.8
KIND_NAMES = ("qkv", "proj", "fcin", "fcout")
KIND_SHAPES = ((D_MODEL, 3 * D_MODEL), (D_MODEL, D_MODEL), (D_MODEL, FF_DIM), (FF_DIM, D_MODEL))


def tilt_profile(num_rows, num_cols):
    row_pos = (jnp.arange(num_rows, dtype=jnp.float32) + 0.5) / num_rows
    col_pos = (jnp.arange(num_cols, dtype=jnp.float32) + 0.5) / num_cols
    row_scale = jnp.exp(TILT_RATE * (2.0 * row_pos - 1.0))
    col_scale = jnp.exp(TILT_RATE * (2.0 * col_pos - 1.0))
    return row_scale[:, None] * col_scale[None, :]


def setup_inputs(seed: int = 0) -> dict:
    base_key = jax.random.key(seed)
    norm_ratio = jax.random.uniform(jax.random.fold_in(base_key, 100), (), jnp.float32, 2.5, 4.5)
    raw_grads = []
    grad_scales = []
    total_sq = jnp.zeros((), jnp.float32)
    for kind_idx, shape_pair in enumerate(KIND_SHAPES):
        num_rows, num_cols = shape_pair
        kind_keys = jax.random.split(jax.random.fold_in(base_key, kind_idx), 7)
        grad_scale = jnp.exp(jax.random.uniform(kind_keys[0], (LAYERS, 1, 1), jnp.float32, -1.1, 1.1))
        common = jax.random.normal(kind_keys[1], (1, LAYERS, num_rows, num_cols), jnp.float32)
        dev_noise = jax.random.normal(kind_keys[2], (DATA_SIZE, LAYERS, num_rows, num_cols), jnp.float32)
        raw_grad = grad_scale * (common + dev_noise)
        mean_grad = jnp.mean(raw_grad, axis=0)
        total_sq = total_sq + jnp.sum(mean_grad * mean_grad)
        raw_grads.append(raw_grad)
        grad_scales.append(grad_scale)
    factor = norm_ratio * MAX_NORM / jnp.sqrt(total_sq)
    inputs = {}
    for kind_idx, shape_pair in enumerate(KIND_SHAPES):
        num_rows, num_cols = shape_pair
        kind_name = KIND_NAMES[kind_idx]
        kind_keys = jax.random.split(jax.random.fold_in(base_key, kind_idx), 7)
        profile = tilt_profile(num_rows, num_cols)
        weight_scale = jnp.exp(jax.random.uniform(kind_keys[3], (LAYERS, 1, 1), jnp.float32, -1.1, 1.1)) * num_rows ** -0.5
        clip_scale = grad_scales[kind_idx] * factor / norm_ratio
        shape_full = (LAYERS, num_rows, num_cols)
        inputs["grad_" + kind_name] = raw_grads[kind_idx] * factor
        inputs["weight_" + kind_name] = jax.random.normal(kind_keys[4], shape_full, jnp.float32) * weight_scale * profile
        inputs["moment1_" + kind_name] = jax.random.normal(kind_keys[5], shape_full, jnp.float32) * clip_scale
        inputs["moment2_" + kind_name] = (clip_scale * profile) ** 2 * jax.random.uniform(kind_keys[6], shape_full, jnp.float32, 0.5, 1.5)
    return inputs


def lamb_tensor(grad_mean, weight, moment1, moment2, clip_coef):
    clipped = clip_coef * grad_mean
    new_first = BETA_ONE * moment1 + (1.0 - BETA_ONE) * clipped
    new_second = BETA_TWO * moment2 + (1.0 - BETA_TWO) * clipped * clipped
    first_hat = new_first / (1.0 - BETA_ONE ** STEP_COUNT)
    second_hat = new_second / (1.0 - BETA_TWO ** STEP_COUNT)
    update = first_hat / (jnp.sqrt(second_hat) + ADAM_EPS) + DECAY_RATE * weight
    weight_norm = jnp.sqrt(jnp.sum(weight * weight, axis=(1, 2), keepdims=True))
    update_norm = jnp.sqrt(jnp.sum(update * update, axis=(1, 2), keepdims=True))
    new_weight = weight - LEARN_RATE * (weight_norm / update_norm) * update
    return new_weight, new_first, new_second


def reference(grad_qkv, weight_qkv, moment1_qkv, moment2_qkv, grad_proj, weight_proj, moment1_proj, moment2_proj, grad_fcin, weight_fcin, moment1_fcin, moment2_fcin, grad_fcout, weight_fcout, moment1_fcout, moment2_fcout):
    grad_list = (grad_qkv, grad_proj, grad_fcin, grad_fcout)
    states = ((weight_qkv, moment1_qkv, moment2_qkv), (weight_proj, moment1_proj, moment2_proj), (weight_fcin, moment1_fcin, moment2_fcin), (weight_fcout, moment1_fcout, moment2_fcout))
    grad_means = [jnp.sum(grad_stack.astype(jnp.bfloat16).astype(jnp.float32), axis=0) / DATA_SIZE for grad_stack in grad_list]
    total_sq = sum(jnp.sum(grad_mean * grad_mean) for grad_mean in grad_means)
    clip_coef = jnp.minimum(1.0, MAX_NORM / jnp.sqrt(total_sq))
    results = [lamb_tensor(grad_means[kind_idx], states[kind_idx][0], states[kind_idx][1], states[kind_idx][2], clip_coef) for kind_idx in range(4)]
    replicas = [outcome[0].astype(jnp.bfloat16) for outcome in results]
    return (replicas[0], replicas[1], replicas[2], replicas[3], results[0][0], results[1][0], results[2][0], results[3][0], results[0][1], results[1][1], results[2][1], results[3][1], results[0][2], results[1][2], results[2][2], results[3][2])
```

```python
import functools

import jax
import jax.numpy as jnp
from jax import lax
from jax.experimental import pallas as pl
from jax.experimental.pallas import tpu as pltpu
from jax.sharding import PartitionSpec as P

LEARN_RATE = 0.08
BETA_ONE = 0.9
BETA_TWO = 0.999
ADAM_EPS = 1e-6
DECAY_RATE = 0.01
MAX_NORM = 1.0
STEP_COUNT = 100
COLUMN_SPLIT = (True, False, True, False)

KINDS = 4
LAYERS = 2
KIND_ORDER = (1, 0, 2, 3)
ME, XN, YN, DG = 0, 1, 2, 3
MESH = pl.DeviceIdType.MESH


def grad_spec(col_split):
    return P("data", None, None, "model") if col_split else P("data", None, "model", None)


def state_spec(col_split):
    return P(None, "data", "model") if col_split else P(None, ("model", "data"), None)


def replica_spec(col_split):
    return P(None, None, "model") if col_split else P(None, "model", None)


def lane_fold(x):
    total = x[:, 0:128]
    for j in range(1, x.shape[1] // 128):
        total = total + x[:, 128 * j:128 * (j + 1)]
    return total


def kernel(n_model, n_data, dims, *refs):
    n_dev = n_model * n_data
    grads, weights, firsts, seconds = (refs[i::4][:KINDS] for i in range(4))
    grads, weights, firsts, seconds = ([refs[4 * k + i] for k in range(KINDS)] for i in range(4))
    outs = refs[16:32]
    replicas, out_w, out_m, out_v = outs[0:4], outs[4:8], outs[8:12], outs[12:16]
    scratch = refs[32:]
    acc, stage, sent, got, p1, p2, wv, mv, vv = (scratch[4 * i:4 * i + 4] for i in range(9))
    (row_a, row_b, all_a, all_b,
     ld_acc, ld_stage, ld_state, d_send, d_recv, p1_send, p1_recv, p2_send, p2_recv,
     g_send, g_recv, h_send, h_recv, st_out, rep_out, ps_send, ps_recv) = scratch[36:]

    model = lax.axis_index("model")
    data = lax.axis_index("data")
    core = data % 2
    xc = (data // 2) % 2
    yc = data // 4
    me = model * n_data + data

    def chip_of(slot):
        x = xc if slot in (ME, YN) else 1 - xc
        y = yc if slot in (ME, XN) else 1 - yc
        return 2 * y + x

    def device(slot, other_core=False):
        return (model, 2 * chip_of(slot) + ((1 - core) if other_core else core))

    partner = device(ME, True)
    to_x = device(XN)
    to_y = device(YN)

    def rows_of(k, slot, other_core):
        rows = dims[k][0]
        return pl.ds(pl.multiple_of((2 * chip_of(slot) + ((1 - core) if other_core else core)) * rows, rows), rows)

    def load_unit(l, s, k):
        return (
            pltpu.make_async_copy(grads[k].at[0, l, rows_of(k, s, True)], stage[k].at[l], ld_stage.at[k, l]),
            pltpu.make_async_copy(grads[k].at[0, l, rows_of(k, s, False)], acc[k].at[l, s], ld_acc.at[k, l, s]),
        )

    def remote(src, dst, send, recv, dev):
        return pltpu.make_async_remote_copy(src_ref=src, dst_ref=dst, send_sem=send, recv_sem=recv, device_id=dev, device_id_type=MESH)

    def pair_copy(l, s, k):
        return remote(sent[k].at[l, s], got[k].at[l, s], d_send.at[k, l, s], d_recv.at[k, l, s], partner)

    first_dev = (to_x, to_y)
    second_dev = (to_y, to_x)
    first_nb = (XN, YN)
    second_nb = (YN, XN)

    def first_copy(l, through, k):
        slot = DG if through else first_nb[l]
        t = 0 if through else 1
        return remote(acc[k].at[l, slot], p1[k].at[l, t], p1_send.at[k, l, t], p1_recv.at[k, l, t], first_dev[l])

    def second_copy(l, k):
        return remote(acc[k].at[l, second_nb[l]], p2[k].at[l], p2_send.at[k, l], p2_recv.at[k, l], second_dev[l])

    def over_rows(k, step, body):
        rows = dims[k][0]

        def run(i, carry):
            body(pl.ds(pl.multiple_of(i * step, step), step))
            return carry

        lax.fori_loop(0, rows // step, run, 0)

    def sum_rows(k, body):
        rows, cols = dims[k]
        return lane_fold(lax.fori_loop(
            0, rows // 8, lambda i, c: c + body(pl.ds(pl.multiple_of(i * 8, 8), 8)), jnp.zeros((8, cols), jnp.float32)))

    units = []
    for slots in ((DG, DG), (YN, XN), (XN, YN), (ME, ME)):
        for k in KIND_ORDER:
            for l in range(LAYERS):
                units.append((l, slots[l], k))
    ahead = 6
    for u in units[:ahead]:
        for c in load_unit(*u):
            c.start()

    barrier = pltpu.get_barrier_semaphore()

    def greet(i, carry):
        t = (me + i) % n_dev
        pl.semaphore_signal(barrier, inc=1, device_id=(t // n_data, t % n_data), device_id_type=MESH)
        return carry

    lax.fori_loop(1, n_dev, greet, 0)
    pl.semaphore_wait(barrier, n_dev - 1)

    def state_load(k):
        return [pltpu.make_async_copy(src[k], dst[k], ld_state.at[i, k]) for i, (src, dst) in enumerate(((weights, wv), (firsts, mv), (seconds, vv)))]

    def pair_half(l, s, k):
        for c in load_unit(l, s, k):
            c.wait()

        def body(r):
            sent[k][l, s, r, :] = stage[k][l, r, :].astype(jnp.bfloat16)

        over_rows(k, 16, body)
        pair_copy(l, s, k).start()

    def chip_half(l, s, k):
        pair_copy(l, s, k).wait_recv()

        def body(r):
            own = acc[k][l, s, r, :].astype(jnp.bfloat16).astype(jnp.float32)
            acc[k][l, s, r, :] = own + got[k][l, s, r, :].astype(jnp.float32)

        over_rows(k, 16, body)
        if s == DG:
            first_copy(l, True, k).start()
        elif s == first_nb[l]:
            first_copy(l, False, k).start()

    lag = 2
    for i in range(len(units) + lag):
        if i < len(units):
            pair_half(*units[i])
            if i + ahead < len(units):
                for c in load_unit(*units[i + ahead]):
                    c.start()
            elif i + ahead - len(units) < KINDS:
                for c in state_load(i + ahead - len(units)):
                    c.start()
        if i >= lag:
            chip_half(*units[i - lag])

    for k in KIND_ORDER:
        for l in range(LAYERS):
            first_copy(l, True, k).wait_recv()
            s = second_nb[l]

            def body(r):
                acc[k][l, s, r, :] = acc[k][l, s, r, :] + p1[k][l, 0, r, :]

            over_rows(k, 8, body)
            second_copy(l, k).start()

    lane = lax.broadcasted_iota(jnp.int32, (1, 128), 1)
    norms = jnp.zeros((1, 128), jnp.float32)
    for k in range(KINDS):
        for c in state_load(k):
            c.wait()
        for l in range(LAYERS):
            part = sum_rows(k, lambda r: wv[k][l, r, :] * wv[k][l, r, :])
            norms = norms + jnp.where(lane == 2 * k + l, jnp.sum(part, keepdims=True), 0.0)

    for k in KIND_ORDER:
        for l in range(LAYERS):
            first_copy(l, False, k).wait_recv()

            def body(r):
                acc[k][l, ME, r, :] = acc[k][l, ME, r, :] + p1[k][l, 1, r, :]

            over_rows(k, 8, body)

    grad_sq = jnp.zeros((8, 128), jnp.float32)
    for k in KIND_ORDER:
        for l in range(LAYERS):
            second_copy(l, k).wait_recv()

            def body(r):
                mean = (acc[k][l, ME, r, :] + p2[k][l, r, :]) * (1.0 / n_data)
                acc[k][l, ME, r, :] = mean
                return mean * mean

            grad_sq = grad_sq + sum_rows(k, body)
    norms = norms + jnp.where(lane == 8, jnp.sum(grad_sq, keepdims=True), 0.0)

    def exchange(which, row_ref, all_ref, row):
        row_ref[...] = row
        all_ref[me] = row

        def send(i, carry):
            t = (me + i) % n_dev
            remote(row_ref, all_ref.at[me], ps_send.at[which], ps_recv.at[which], (t // n_data, t % n_data)).start()
            return carry

        lax.fori_loop(1, n_dev, send, 0)
        rest = all_ref.at[pl.ds(0, n_dev - 1)]
        pltpu.make_async_copy(rest, rest, ps_recv.at[which]).wait()
        return jnp.sum(all_ref[...], axis=0)

    norms = exchange(0, row_a, all_a, norms)

    def pick(row, i):
        return jnp.sum(jnp.where(lane == i, row, 0.0), axis=1, keepdims=True)

    clip = jnp.minimum(1.0, MAX_NORM / jnp.sqrt(pick(norms, 8)))

    squares = jnp.zeros((1, 128), jnp.float32)
    for k in KIND_ORDER:
        for l in range(LAYERS):

            def body(r):
                clipped = clip * acc[k][l, ME, r, :]
                weight = wv[k][l, r, :]
                first = BETA_ONE * mv[k][l, r, :] + (1.0 - BETA_ONE) * clipped
                second = BETA_TWO * vv[k][l, r, :] + (1.0 - BETA_TWO) * clipped * clipped
                mv[k][l, r, :] = first
                vv[k][l, r, :] = second
                first_hat = first * (1.0 / (1.0 - BETA_ONE ** STEP_COUNT))
                second_hat = second * (1.0 / (1.0 - BETA_TWO ** STEP_COUNT))
                update = first_hat / (jnp.sqrt(second_hat) + ADAM_EPS) + DECAY_RATE * weight
                acc[k][l, ME, r, :] = update
                return update * update

            part = sum_rows(k, body)
            squares = squares + jnp.where(lane == 2 * k + l, jnp.sum(part, keepdims=True), 0.0)

    for (l, s, k) in units:
        pair_copy(l, s, k).wait_send()
    for k in range(KINDS):
        for l in range(LAYERS):
            first_copy(l, True, k).wait_send()
            first_copy(l, False, k).wait_send()
            second_copy(l, k).wait_send()

    squares = exchange(1, row_b, all_b, squares)
    for k in range(KINDS):
        pltpu.make_async_copy(mv[k], out_m[k], st_out.at[1, k]).start()
        pltpu.make_async_copy(vv[k], out_v[k], st_out.at[2, k]).start()
    ratios = jnp.sqrt(norms) / jnp.sqrt(squares)

    def own_copy(l, along, k):
        return remote(sent[k].at[l, ME], sent[k].at[l, along], g_send.at[k, l, along], g_recv.at[k, l, along], to_x if along == XN else to_y)

    def pass_copy(l, k):
        return remote(sent[k].at[l, first_nb[l]], sent[k].at[l, DG], g_send.at[k, l, DG], g_recv.at[k, l, DG], second_dev[l])

    def half_copy(l, s, k):
        return remote(sent[k].at[l, s], got[k].at[l, s], h_send.at[k, l, s], h_recv.at[k, l, s], partner)

    def write(l, s, k, other_core):
        src = got if other_core else sent
        pltpu.make_async_copy(src[k].at[l, s], replicas[k].at[l, rows_of(k, s, other_core)], rep_out.at[k]).start()

    pending = []

    def spread(l, s, k):
        half_copy(l, s, k).start()
        write(l, s, k, False)
        pending.append((l, s, k))

    def collect(keep):
        while len(pending) > keep:
            l, s, k = pending.pop(0)
            half_copy(l, s, k).wait_recv()
            write(l, s, k, True)

    for k in KIND_ORDER:
        for l in range(LAYERS):
            scale = LEARN_RATE * pick(ratios, 2 * k + l)

            def body(r):
                fresh = wv[k][l, r, :] - scale * acc[k][l, ME, r, :]
                wv[k][l, r, :] = fresh
                sent[k][l, ME, r, :] = fresh.astype(jnp.bfloat16)

            over_rows(k, 16, body)
            own_copy(l, first_nb[l], k).start()
    for k in KIND_ORDER:
        for l in range(LAYERS):
            own_copy(l, second_nb[l], k).start()
            spread(l, ME, k)
        pltpu.make_async_copy(wv[k], out_w[k], st_out.at[0, k]).start()

    for k in KIND_ORDER:
        for l in range(LAYERS):
            own_copy(l, first_nb[l], k).wait_recv()
            pass_copy(l, k).start()
            spread(l, first_nb[l], k)
            collect(2)
    for k in KIND_ORDER:
        for l in range(LAYERS):
            own_copy(l, second_nb[l], k).wait_recv()
            spread(l, second_nb[l], k)
            collect(2)
    for k in KIND_ORDER:
        for l in range(LAYERS):
            pass_copy(l, k).wait_recv()
            spread(l, DG, k)
            collect(2)
    collect(0)

    for k in range(KINDS):
        for l in range(LAYERS):
            own_copy(l, XN, k).wait_send()
            own_copy(l, YN, k).wait_send()
            pass_copy(l, k).wait_send()
            for s in range(4):
                half_copy(l, s, k).wait_send()
    for which, all_ref in ((0, all_a), (1, all_b)):
        rest = all_ref.at[pl.ds(0, n_dev - 1)]
        pltpu.make_async_copy(rest, rest, ps_send.at[which]).wait()
    for k in range(KINDS):
        pltpu.make_async_copy(replicas[k], replicas[k], rep_out.at[k]).wait()
        pltpu.make_async_copy(wv[k], out_w[k], st_out.at[0, k]).wait()
        pltpu.make_async_copy(mv[k], out_m[k], st_out.at[1, k]).wait()
        pltpu.make_async_copy(vv[k], out_v[k], st_out.at[2, k]).wait()


def solution(mesh):
    n_model, n_data = mesh.shape["model"], mesh.shape["data"]
    in_specs = []
    for col_split in COLUMN_SPLIT:
        in_specs.extend([grad_spec(col_split), state_spec(col_split), state_spec(col_split), state_spec(col_split)])
    out_specs = tuple([replica_spec(col_split) for col_split in COLUMN_SPLIT] + [state_spec(col_split) for col_split in COLUMN_SPLIT] * 3)

    def device_step(*arrays):
        dims = [arrays[4 * k + 1].shape[1:] for k in range(KINDS)]
        f32, bf16 = jnp.float32, jnp.bfloat16
        out_shape = [jax.ShapeDtypeStruct((LAYERS, n_data * d[0], d[1]), bf16) for d in dims]
        out_shape += [jax.ShapeDtypeStruct((LAYERS,) + tuple(d), f32) for d in dims] * 3

        def each(prefix, dtype):
            return [pltpu.VMEM(prefix + tuple(d), dtype) for d in dims]

        dma = pltpu.SemaphoreType.DMA
        n_dev = n_model * n_data
        scratch = (each((LAYERS, 4), f32) + each((LAYERS,), f32) + each((LAYERS, 4), bf16) + each((LAYERS, 4), bf16)
                   + each((LAYERS, 2), f32) + each((LAYERS,), f32) + each((LAYERS,), f32) * 3)
        scratch += [pltpu.VMEM((1, 128), f32), pltpu.VMEM((1, 128), f32), pltpu.VMEM((n_dev, 1, 128), f32), pltpu.VMEM((n_dev, 1, 128), f32)]
        scratch += [dma((4, 2, 4)), dma((4, 2)), dma((3, 4)), dma((4, 2, 4)), dma((4, 2, 4)), dma((4, 2, 2)), dma((4, 2, 2)), dma((4, 2)), dma((4, 2)),
                    dma((4, 2, 4)), dma((4, 2, 4)), dma((4, 2, 4)), dma((4, 2, 4)), dma((3, 4)), dma((4,)), dma((2,)), dma((2,))]
        return tuple(pl.pallas_call(
            functools.partial(kernel, n_model, n_data, dims),
            out_shape=out_shape,
            in_specs=[pl.BlockSpec(memory_space=pl.ANY)] * 16,
            out_specs=[pl.BlockSpec(memory_space=pl.ANY)] * 16,
            scratch_shapes=scratch,
            compiler_params=pltpu.CompilerParams(collective_id=0, has_side_effects=True, vmem_limit_bytes=60 * 1024 * 1024),
            name="lamb_step",
        )(*arrays))

    return jax.shard_map(device_step, mesh=mesh, in_specs=tuple(in_specs), out_specs=out_specs, check_vma=False)
```

```python
import functools

import jax
import jax.numpy as jnp
from jax import lax
from jax.experimental import pallas as pl
from jax.experimental.pallas import tpu as pltpu
from jax.sharding import PartitionSpec as P

LEARN_RATE = 0.08
BETA_ONE = 0.9
BETA_TWO = 0.999
ADAM_EPS = 1e-6
DECAY_RATE = 0.01
MAX_NORM = 1.0
STEP_COUNT = 100
COLUMN_SPLIT = (True, False, True, False)

KINDS = 4
LAYERS = 2
KIND_ORDER = (1, 0, 2, 3)
ME, XN, YN, DG = 0, 1, 2, 3
MESH = pl.DeviceIdType.MESH
COMM_VMEM = 42 << 20


def grad_spec(col_split):
    return P("data", None, None, "model") if col_split else P("data", None, "model", None)


def state_spec(col_split):
    return P(None, "data", "model") if col_split else P(None, ("model", "data"), None)


def replica_spec(col_split):
    return P(None, None, "model") if col_split else P(None, "model", None)


def lane_fold(x):
    total = x[:, 0:128]
    for j in range(1, x.shape[1] // 128):
        total = total + x[:, 128 * j:128 * (j + 1)]
    return total


def kernel(n_model, n_data, dims, *refs):
    n_dev = n_model * n_data
    grads, weights, firsts, seconds = ([refs[4 * k + i] for k in range(KINDS)] for i in range(4))
    outs = refs[16:32]
    replicas, wv, mv, vv = outs[0:4], outs[4:8], outs[8:12], outs[12:16]
    scratch = refs[32:]
    acc, stage, sent, got, p1, p2 = (scratch[4 * i:4 * i + 4] for i in range(6))
    (row_a, row_b, all_a, all_b,
     ld_acc, ld_stage, ld_state, d_send, d_recv, p1_send, p1_recv, p2_send, p2_recv,
     g_send, g_recv, h_send, h_recv, ps_send, ps_recv) = scratch[24:]

    model = lax.axis_index("model")
    data = lax.axis_index("data")
    core = data % 2
    xc = (data // 2) % 2
    yc = data // 4
    me = model * n_data + data

    def chip_of(slot):
        x = xc if slot in (ME, YN) else 1 - xc
        y = yc if slot in (ME, XN) else 1 - yc
        return 2 * y + x

    def device(slot, other_core=False):
        return (model, 2 * chip_of(slot) + ((1 - core) if other_core else core))

    partner = device(ME, True)
    to_x = device(XN)
    to_y = device(YN)

    def rows_of(k, slot, other_core):
        rows = dims[k][0]
        return pl.ds(pl.multiple_of((2 * chip_of(slot) + ((1 - core) if other_core else core)) * rows, rows), rows)

    def load_unit(l, s, k):
        return (
            pltpu.make_async_copy(grads[k].at[0, l, rows_of(k, s, True)], stage[k].at[l], ld_stage.at[k, l]),
            pltpu.make_async_copy(grads[k].at[0, l, rows_of(k, s, False)], acc[k].at[l, s], ld_acc.at[k, l, s]),
        )

    def remote(src, dst, send, recv, dev):
        return pltpu.make_async_remote_copy(src_ref=src, dst_ref=dst, send_sem=send, recv_sem=recv, device_id=dev, device_id_type=MESH)

    def pair_copy(l, s, k):
        return remote(sent[k].at[l, s], got[k].at[l, s], d_send.at[k, l, s], d_recv.at[k, l, s], partner)

    first_dev = (to_x, to_y)
    second_dev = (to_y, to_x)
    first_nb = (XN, YN)
    second_nb = (YN, XN)

    def first_copy(l, through, k):
        slot = DG if through else first_nb[l]
        t = 0 if through else 1
        return remote(acc[k].at[l, slot], p1[k].at[l, t], p1_send.at[k, l, t], p1_recv.at[k, l, t], first_dev[l])

    def second_copy(l, k):
        return remote(acc[k].at[l, second_nb[l]], p2[k].at[l], p2_send.at[k, l], p2_recv.at[k, l], second_dev[l])

    def over_rows(k, step, body):
        rows = dims[k][0]

        def run(i, carry):
            body(pl.ds(pl.multiple_of(i * step, step), step))
            return carry

        lax.fori_loop(0, rows // step, run, 0)

    def sum_rows(k, body):
        rows, cols = dims[k]
        return lane_fold(lax.fori_loop(
            0, rows // 8, lambda i, c: c + body(pl.ds(pl.multiple_of(i * 8, 8), 8)), jnp.zeros((8, cols), jnp.float32)))

    units = []
    for slots in ((DG, DG), (YN, XN), (XN, YN), (ME, ME)):
        for k in KIND_ORDER:
            for l in range(LAYERS):
                units.append((l, slots[l], k))
    ahead = 6
    for u in units[:ahead]:
        for c in load_unit(*u):
            c.start()

    barrier = pltpu.get_barrier_semaphore()

    def greet(i, carry):
        t = (me + i) % n_dev
        pl.semaphore_signal(barrier, inc=1, device_id=(t // n_data, t % n_data), device_id_type=MESH)
        return carry

    lax.fori_loop(1, n_dev, greet, 0)
    pl.semaphore_wait(barrier, n_dev - 1)

    def state_load(k):
        return [pltpu.make_async_copy(src[k], dst[k], ld_state.at[i, k]) for i, (src, dst) in enumerate(((weights, wv), (firsts, mv), (seconds, vv)))]

    def pair_half(l, s, k):
        for c in load_unit(l, s, k):
            c.wait()

        def body(r):
            sent[k][l, s, r, :] = stage[k][l, r, :].astype(jnp.bfloat16)

        over_rows(k, 16, body)
        pair_copy(l, s, k).start()

    def chip_half(l, s, k):
        pair_copy(l, s, k).wait_recv()

        def body(r):
            own = acc[k][l, s, r, :].astype(jnp.bfloat16).astype(jnp.float32)
            acc[k][l, s, r, :] = own + got[k][l, s, r, :].astype(jnp.float32)

        over_rows(k, 16, body)
        if s == DG:
            first_copy(l, True, k).start()
        elif s == first_nb[l]:
            first_copy(l, False, k).start()

    lag = 2
    for i in range(len(units) + lag):
        if i < len(units):
            pair_half(*units[i])
            if i + ahead < len(units):
                for c in load_unit(*units[i + ahead]):
                    c.start()
            elif i + ahead - len(units) < KINDS:
                for c in state_load(i + ahead - len(units)):
                    c.start()
        if i >= lag:
            chip_half(*units[i - lag])

    for k in KIND_ORDER:
        for l in range(LAYERS):
            first_copy(l, True, k).wait_recv()
            s = second_nb[l]

            def body(r):
                acc[k][l, s, r, :] = acc[k][l, s, r, :] + p1[k][l, 0, r, :]

            over_rows(k, 8, body)
            second_copy(l, k).start()

    lane = lax.broadcasted_iota(jnp.int32, (1, 128), 1)
    norms = jnp.zeros((1, 128), jnp.float32)
    for k in range(KINDS):
        for c in state_load(k):
            c.wait()
        for l in range(LAYERS):
            part = sum_rows(k, lambda r: wv[k][l, r, :] * wv[k][l, r, :])
            norms = norms + jnp.where(lane == 2 * k + l, jnp.sum(part, keepdims=True), 0.0)

    for k in KIND_ORDER:
        for l in range(LAYERS):
            first_copy(l, False, k).wait_recv()

            def body(r):
                acc[k][l, ME, r, :] = acc[k][l, ME, r, :] + p1[k][l, 1, r, :]

            over_rows(k, 8, body)

    grad_sq = jnp.zeros((8, 128), jnp.float32)
    for k in KIND_ORDER:
        for l in range(LAYERS):
            second_copy(l, k).wait_recv()

            def body(r):
                mean = (acc[k][l, ME, r, :] + p2[k][l, r, :]) * (1.0 / n_data)
                acc[k][l, ME, r, :] = mean
                return mean * mean

            grad_sq = grad_sq + sum_rows(k, body)
    norms = norms + jnp.where(lane == 8, jnp.sum(grad_sq, keepdims=True), 0.0)

    def exchange(which, row_ref, all_ref, row):
        row_ref[...] = row
        all_ref[me] = row

        def send(i, carry):
            t = (me + i) % n_dev
            remote(row_ref, all_ref.at[me], ps_send.at[which], ps_recv.at[which], (t // n_data, t % n_data)).start()
            return carry

        lax.fori_loop(1, n_dev, send, 0)
        rest = all_ref.at[pl.ds(0, n_dev - 1)]
        pltpu.make_async_copy(rest, rest, ps_recv.at[which]).wait()
        return jnp.sum(all_ref[...], axis=0)

    norms = exchange(0, row_a, all_a, norms)

    def pick(row, i):
        return jnp.sum(jnp.where(lane == i, row, 0.0), axis=1, keepdims=True)

    clip = jnp.minimum(1.0, MAX_NORM / jnp.sqrt(pick(norms, 8)))

    squares = jnp.zeros((1, 128), jnp.float32)
    for k in KIND_ORDER:
        for l in range(LAYERS):

            def body(r):
                clipped = clip * acc[k][l, ME, r, :]
                weight = wv[k][l, r, :]
                first = BETA_ONE * mv[k][l, r, :] + (1.0 - BETA_ONE) * clipped
                second = BETA_TWO * vv[k][l, r, :] + (1.0 - BETA_TWO) * clipped * clipped
                mv[k][l, r, :] = first
                vv[k][l, r, :] = second
                first_hat = first * (1.0 / (1.0 - BETA_ONE ** STEP_COUNT))
                second_hat = second * (1.0 / (1.0 - BETA_TWO ** STEP_COUNT))
                update = first_hat / (jnp.sqrt(second_hat) + ADAM_EPS) + DECAY_RATE * weight
                acc[k][l, ME, r, :] = update
                return update * update

            part = sum_rows(k, body)
            squares = squares + jnp.where(lane == 2 * k + l, jnp.sum(part, keepdims=True), 0.0)

    squares = exchange(1, row_b, all_b, squares)
    ratios = jnp.sqrt(norms) / jnp.sqrt(squares)

    def block(l, s, k):
        return replicas[k].at[l, rows_of(k, s, False)]

    def own_copy(l, along, k):
        return remote(block(l, ME, k), block(l, ME, k), g_send.at[k, l, along], g_recv.at[k, l, along], to_x if along == XN else to_y)

    def pass_copy(l, k):
        src = block(l, first_nb[l], k)
        return remote(src, src, g_send.at[k, l, DG], g_recv.at[k, l, DG], second_dev[l])

    def half_copy(l, s, k):
        return remote(block(l, s, k), block(l, s, k), h_send.at[k, l, s], h_recv.at[k, l, s], partner)

    for k in KIND_ORDER:
        for l in range(LAYERS):
            scale = LEARN_RATE * pick(ratios, 2 * k + l)
            start = pl.multiple_of(data * dims[k][0], dims[k][0])

            def body(r, at):
                fresh = wv[k][l, r, :] - scale * acc[k][l, ME, r, :]
                wv[k][l, r, :] = fresh
                replicas[k][l, pl.ds(pl.multiple_of(start + at, 16), 16), :] = fresh.astype(jnp.bfloat16)

            lax.fori_loop(0, dims[k][0] // 16, lambda i, c: (body(pl.ds(pl.multiple_of(i * 16, 16), 16), i * 16), c)[1], 0)
            own_copy(l, first_nb[l], k).start()
    for k in KIND_ORDER:
        for l in range(LAYERS):
            own_copy(l, second_nb[l], k).start()
            half_copy(l, ME, k).start()

    for k in KIND_ORDER:
        for l in range(LAYERS):
            own_copy(l, first_nb[l], k).wait_recv()
            pass_copy(l, k).start()
            half_copy(l, first_nb[l], k).start()
    for k in KIND_ORDER:
        for l in range(LAYERS):
            own_copy(l, second_nb[l], k).wait_recv()
            half_copy(l, second_nb[l], k).start()
    for k in KIND_ORDER:
        for l in range(LAYERS):
            pass_copy(l, k).wait_recv()
            half_copy(l, DG, k).start()

    for (l, s, k) in units:
        pair_copy(l, s, k).wait_send()
    for k in range(KINDS):
        for l in range(LAYERS):
            first_copy(l, True, k).wait_send()
            first_copy(l, False, k).wait_send()
            second_copy(l, k).wait_send()

    for k in range(KINDS):
        for l in range(LAYERS):
            own_copy(l, XN, k).wait_send()
            own_copy(l, YN, k).wait_send()
            pass_copy(l, k).wait_send()
            for s in range(4):
                half_copy(l, s, k).wait()
    for which, all_ref in ((0, all_a), (1, all_b)):
        rest = all_ref.at[pl.ds(0, n_dev - 1)]
        pltpu.make_async_copy(rest, rest, ps_send.at[which]).wait()

def write_out(count, *refs):
    srcs, dsts, sems = refs[:count], refs[count:2 * count], refs[2 * count]
    copies = [pltpu.make_async_copy(src, dst, sems.at[i]) for i, (src, dst) in enumerate(zip(srcs, dsts))]
    for c in copies:
        c.start()
    for c in copies:
        c.wait()


def solution(mesh):
    n_model, n_data = mesh.shape["model"], mesh.shape["data"]
    in_specs = []
    for col_split in COLUMN_SPLIT:
        in_specs.extend([grad_spec(col_split), state_spec(col_split), state_spec(col_split), state_spec(col_split)])
    out_specs = tuple([replica_spec(col_split) for col_split in COLUMN_SPLIT] + [state_spec(col_split) for col_split in COLUMN_SPLIT] * 3)

    def device_step(*arrays):
        dims = [arrays[4 * k + 1].shape[1:] for k in range(KINDS)]
        f32, bf16 = jnp.float32, jnp.bfloat16
        out_shape = [jax.ShapeDtypeStruct((LAYERS, n_data * d[0], d[1]), bf16) for d in dims]
        out_shape += [jax.ShapeDtypeStruct((LAYERS,) + tuple(d), f32) for d in dims] * 3

        def each(prefix, dtype):
            return [pltpu.VMEM(prefix + tuple(d), dtype) for d in dims]

        dma = pltpu.SemaphoreType.DMA
        n_dev = n_model * n_data
        scratch = (each((LAYERS, 4), f32) + each((LAYERS,), f32) + each((LAYERS, 4), bf16) + each((LAYERS, 4), bf16)
                   + each((LAYERS, 2), f32) + each((LAYERS,), f32))
        scratch += [pltpu.VMEM((1, 128), f32), pltpu.VMEM((1, 128), f32), pltpu.VMEM((n_dev, 1, 128), f32), pltpu.VMEM((n_dev, 1, 128), f32)]
        scratch += [dma((4, 2, 4)), dma((4, 2)), dma((3, 4)), dma((4, 2, 4)), dma((4, 2, 4)), dma((4, 2, 2)), dma((4, 2, 2)), dma((4, 2)), dma((4, 2)),
                    dma((4, 2, 4)), dma((4, 2, 4)), dma((4, 2, 4)), dma((4, 2, 4)), dma((2,)), dma((2,))]
        held = pl.pallas_call(
            functools.partial(kernel, n_model, n_data, dims),
            out_shape=[pltpu.VMEM(o.shape, o.dtype) for o in out_shape],
            in_specs=[pl.BlockSpec(memory_space=pl.ANY)] * 16,
            out_specs=[pl.BlockSpec(memory_space=pltpu.VMEM)] * 16,
            scratch_shapes=scratch,
            compiler_params=pltpu.CompilerParams(collective_id=0, has_side_effects=True, vmem_limit_bytes=COMM_VMEM),
            name="lamb_step",
        )(*arrays)
        held = [pltpu.with_memory_space_constraint(h, pltpu.VMEM) for h in held]
        return tuple(pl.pallas_call(
            functools.partial(write_out, len(out_shape)),
            out_shape=out_shape,
            in_specs=[pl.BlockSpec(memory_space=pltpu.VMEM)] * 16,
            out_specs=[pl.BlockSpec(memory_space=pl.ANY)] * 16,
            scratch_shapes=[dma((16,))],
            compiler_params=pltpu.CompilerParams(vmem_limit_bytes=1 << 20),
            name="write_out",
        )(*held))

    return jax.shard_map(device_step, mesh=mesh, in_specs=tuple(in_specs), out_specs=out_specs, check_vma=False)
```

```python
import functools

import jax
import jax.numpy as jnp
from jax import lax
from jax.experimental import pallas as pl
from jax.experimental.pallas import tpu as pltpu
from jax.sharding import PartitionSpec as P

LEARN_RATE = 0.08
BETA_ONE = 0.9
BETA_TWO = 0.999
ADAM_EPS = 1e-6
DECAY_RATE = 0.01
MAX_NORM = 1.0
STEP_COUNT = 100
COLUMN_SPLIT = (True, False, True, False)

KINDS = 4
LAYERS = 2
KIND_ORDER = (1, 0, 2, 3)
ME, XN, YN, DG = 0, 1, 2, 3
MESH = pl.DeviceIdType.MESH
COMM_VMEM = 42 << 20


def grad_spec(col_split):
    return P("data", None, None, "model") if col_split else P("data", None, "model", None)


def state_spec(col_split):
    return P(None, "data", "model") if col_split else P(None, ("model", "data"), None)


def replica_spec(col_split):
    return P(None, None, "model") if col_split else P(None, "model", None)


def lane_fold(x):
    total = x[:, 0:128]
    for j in range(1, x.shape[1] // 128):
        total = total + x[:, 128 * j:128 * (j + 1)]
    return total


def kernel(n_model, n_data, dims, *refs):
    n_dev = n_model * n_data
    grads, weights, firsts, seconds = ([refs[4 * k + i] for k in range(KINDS)] for i in range(4))
    outs = refs[16:32]
    replicas, wv, mv, vv = outs[0:4], outs[4:8], outs[8:12], outs[12:16]
    scratch = refs[32:]
    acc, stage, sent, got, p1, p2 = (scratch[4 * i:4 * i + 4] for i in range(6))
    (row_ref, all_ref, ld_unit, ld_state, d_send, d_recv, p1_send, p1_recv, p2_send, p2_recv,
     g_send, g_recv, h_send, h_recv, ps_send, ps_recv, rounds) = scratch[24:]

    model = lax.axis_index("model")
    data = lax.axis_index("data")
    core = data % 2
    xc = (data // 2) % 2
    yc = data // 4
    me = model * n_data + data

    def chip_of(slot):
        x = xc if slot in (ME, YN) else 1 - xc
        y = yc if slot in (ME, XN) else 1 - yc
        return 2 * y + x

    def device(slot, other_core=False):
        return (model, 2 * chip_of(slot) + ((1 - core) if other_core else core))

    partner = device(ME, True)
    to_x = device(XN)
    to_y = device(YN)

    def rows_of(k, slot, other_core):
        rows = dims[k][0]
        return pl.ds(pl.multiple_of((2 * chip_of(slot) + ((1 - core) if other_core else core)) * rows, rows), rows)

    def load_unit(l, s, k):
        pltpu.make_async_copy(grads[k].at[0, l, rows_of(k, s, True)], stage[k].at[l], ld_unit.at[k, l]).start()
        pltpu.make_async_copy(grads[k].at[0, l, rows_of(k, s, False)], acc[k].at[l, s], ld_unit.at[k, l]).start()

    def remote(src, dst, send, recv, dev):
        return pltpu.make_async_remote_copy(src_ref=src, dst_ref=dst, send_sem=send, recv_sem=recv, device_id=dev, device_id_type=MESH)

    def await_bytes(ref, sem):
        pltpu.make_async_copy(ref, ref, sem).wait()

    first_dev = (to_x, to_y)
    second_dev = (to_y, to_x)
    first_nb = (XN, YN)
    second_nb = (YN, XN)

    def over_rows(k, step, body):
        def run(i, carry):
            body(pl.ds(pl.multiple_of(i * step, step), step))
            return carry

        lax.fori_loop(0, dims[k][0] // step, run, 0)

    def sum_rows(k, body):
        rows, cols = dims[k]
        return lane_fold(lax.fori_loop(
            0, rows // 8, lambda i, c: c + body(pl.ds(pl.multiple_of(i * 8, 8), 8)), jnp.zeros((8, cols), jnp.float32)))

    pairs = [(slots, k) for slots in ((DG, DG), (YN, XN), (XN, YN), (ME, ME)) for k in KIND_ORDER]
    ahead = 3

    def load_pair(slots, k):
        for l in range(LAYERS):
            load_unit(l, slots[l], k)

    for p in pairs[:ahead]:
        load_pair(*p)

    barrier = pltpu.get_barrier_semaphore()
    hops = 3 + jnp.minimum(model, 1) + jnp.minimum(n_model - 1 - model, 1)

    def greet(sem):
        for dev in (partner, to_x, to_y):
            pl.semaphore_signal(sem, inc=1, device_id=dev, device_id_type=MESH)

        @pl.when(model > 0)
        def _():
            pl.semaphore_signal(sem, inc=1, device_id=(model - 1, data), device_id_type=MESH)

        @pl.when(model < n_model - 1)
        def _():
            pl.semaphore_signal(sem, inc=1, device_id=(model + 1, data), device_id_type=MESH)

    greet(barrier)
    pl.semaphore_wait(barrier, hops)
    n_rounds = 2 + n_model - 1
    greet(rounds.at[0])

    def next_round(r):
        pl.semaphore_wait(rounds.at[r], hops)
        if r + 1 < n_rounds:
            greet(rounds.at[r + 1])

    def load_state(k):
        for src, dst in ((weights, wv), (firsts, mv), (seconds, vv)):
            pltpu.make_async_copy(src[k], dst[k], ld_state.at[k]).start()

    def pair_half(g, slots, k):
        for l in range(LAYERS):
            await_bytes(acc[k].at[l, pl.ds(0, 2)], ld_unit.at[k, l])
            s = slots[l]

            def body(r):
                sent[k][l, s, r, :] = stage[k][l, r, :].astype(jnp.bfloat16)

            over_rows(k, 16, body)
            remote(sent[k].at[l, s], got[k].at[l, s], d_send.at[k], d_recv.at[g, k], partner).start()

    def chip_half(g, slots, k):
        await_bytes(got[k].at[pl.ds(0, LAYERS), 0], d_recv.at[g, k])
        for l in range(LAYERS):
            s = slots[l]

            def body(r):
                own = acc[k][l, s, r, :].astype(jnp.bfloat16).astype(jnp.float32)
                acc[k][l, s, r, :] = own + got[k][l, s, r, :].astype(jnp.float32)

            over_rows(k, 16, body)
            if s == DG or s == first_nb[l]:
                t = 0 if s == DG else 1
                remote(acc[k].at[l, s], p1[k].at[l, t], p1_send.at[k], p1_recv.at[t, k], first_dev[l]).start()

    for i in range(len(pairs) + 1):
        if i < len(pairs):
            pair_half(i // KINDS, *pairs[i])
            if i + ahead < len(pairs):
                load_pair(*pairs[i + ahead])
            else:
                for k in (KIND_ORDER[i + ahead - len(pairs)],) + ((KIND_ORDER[ahead],) if i + 1 == len(pairs) else ()):
                    load_state(k)
        if i >= 1:
            chip_half((i - 1) // KINDS, *pairs[i - 1])
        if i >= 4 and i % 2 == 0 and (i - 4) // 2 < n_rounds:
            next_round((i - 4) // 2)

    for k in KIND_ORDER:
        await_bytes(p1[k].at[pl.ds(0, LAYERS), 0], p1_recv.at[0, k])
        for l in range(LAYERS):
            s = second_nb[l]

            def body(r):
                acc[k][l, s, r, :] = acc[k][l, s, r, :] + p1[k][l, 0, r, :]

            over_rows(k, 8, body)
            remote(acc[k].at[l, s], p2[k].at[l], p2_send.at[k], p2_recv.at[k], second_dev[l]).start()

    def share(which, row):
        row_ref[which] = row
        all_ref[which, me] = row
        for dz in sorted(range(n_model), key=lambda z: -min(z, n_model - z)):
            for dd in reversed(range(n_data)):
                if dz or dd:
                    remote(row_ref.at[which], all_ref.at[which, me], ps_send.at[which], ps_recv.at[which],
                           ((model + dz) % n_model, (data + dd) % n_data)).start()

    def shared(which):
        await_bytes(all_ref.at[which, pl.ds(0, n_dev - 1)], ps_recv.at[which])
        return jnp.sum(all_ref[which], axis=0)

    lane = lax.broadcasted_iota(jnp.int32, (1, 128), 1)

    def put(i, part):
        return jnp.where(lane == i, jnp.sum(part, keepdims=True), 0.0)

    def pick(row, i):
        return jnp.sum(jnp.where(lane == i, row, 0.0), axis=1, keepdims=True)

    norms = jnp.zeros((1, 128), jnp.float32)
    for k in KIND_ORDER:
        await_bytes(acc[k].at[pl.ds(0, LAYERS), pl.ds(0, 3)], ld_state.at[k])
        for l in range(LAYERS):
            norms = norms + put(2 * k + l, sum_rows(k, lambda r: wv[k][l, r, :] * wv[k][l, r, :]))
    share(5, norms)

    for k in KIND_ORDER:
        await_bytes(p1[k].at[pl.ds(0, LAYERS), 0], p1_recv.at[1, k])
        for l in range(LAYERS):

            def body(r):
                acc[k][l, ME, r, :] = acc[k][l, ME, r, :] + p1[k][l, 1, r, :]

            over_rows(k, 8, body)
    weight_norms = jnp.sqrt(shared(5))

    grad_sq = jnp.zeros((8, 128), jnp.float32)
    for k in KIND_ORDER:
        await_bytes(p2[k], p2_recv.at[k])
        for l in range(LAYERS):

            def body(r):
                mean = (acc[k][l, ME, r, :] + p2[k][l, r, :]) * (1.0 / n_data)
                acc[k][l, ME, r, :] = mean
                return mean * mean

            grad_sq = grad_sq + sum_rows(k, body)
    share(4, jnp.sum(grad_sq, axis=0, keepdims=True))
    total_sq = jnp.sum(shared(4), axis=1, keepdims=True)
    clip = jnp.minimum(1.0, MAX_NORM / jnp.sqrt(total_sq))
    first_gain = (1.0 - BETA_ONE) * clip
    second_gain = (1.0 - BETA_TWO) * clip * clip
    root_scale = (1.0 - BETA_TWO ** STEP_COUNT) ** 0.5
    hat_scale = root_scale / (1.0 - BETA_ONE ** STEP_COUNT)

    for k in KIND_ORDER:
        squares = jnp.zeros((1, 128), jnp.float32)
        for l in range(LAYERS):

            def body(r):
                mean = acc[k][l, ME, r, :]
                first = BETA_ONE * mv[k][l, r, :] + first_gain * mean
                second = BETA_TWO * vv[k][l, r, :] + second_gain * (mean * mean)
                mv[k][l, r, :] = first
                vv[k][l, r, :] = second
                update = (hat_scale * first) / (jnp.sqrt(second) + ADAM_EPS * root_scale) + DECAY_RATE * wv[k][l, r, :]
                acc[k][l, ME, r, :] = update
                return update * update

            squares = squares + put(2 * k + l, sum_rows(k, body))
        share(k, squares)

    def block(l, s, k):
        return replicas[k].at[l, rows_of(k, s, False)]

    def own_copy(l, second, k):
        return remote(block(l, ME, k), block(l, ME, k), g_send.at[k], g_recv.at[second, k], second_dev[l] if second else first_dev[l])

    def pass_copy(l, k):
        src = block(l, first_nb[l], k)
        return remote(src, src, g_send.at[k], g_recv.at[2, k], second_dev[l])

    def half_copy(l, s, k):
        return remote(block(l, s, k), block(l, s, k), h_send.at[k], h_recv.at[k], partner)

    def await_blocks(i, k):
        await_bytes(got[k].at[pl.ds(0, LAYERS), 0], g_recv.at[i, k])

    for k in KIND_ORDER:
        ratios = weight_norms / jnp.sqrt(shared(k))
        for l in range(LAYERS):
            scale = LEARN_RATE * pick(ratios, 2 * k + l)
            start = pl.multiple_of(data * dims[k][0], dims[k][0])

            def body(r, at):
                fresh = wv[k][l, r, :] - scale * acc[k][l, ME, r, :]
                wv[k][l, r, :] = fresh
                replicas[k][l, pl.ds(pl.multiple_of(start + at, 16), 16), :] = fresh.astype(jnp.bfloat16)

            lax.fori_loop(0, dims[k][0] // 16, lambda i, c: (body(pl.ds(pl.multiple_of(i * 16, 16), 16), i * 16), c)[1], 0)
            own_copy(l, 0, k).start()
    for k in KIND_ORDER:
        for l in range(LAYERS):
            own_copy(l, 1, k).start()
            half_copy(l, ME, k).start()

    last = KIND_ORDER[0]
    for k in KIND_ORDER:
        await_blocks(0, k)
        for l in range(LAYERS):
            if k != last:
                pass_copy(l, k).start()
            half_copy(l, first_nb[l], k).start()
    for l in range(LAYERS):
        pass_copy(l, last).start()
    for k in KIND_ORDER:
        await_blocks(1, k)
        for l in range(LAYERS):
            half_copy(l, second_nb[l], k).start()
    for k in KIND_ORDER[1:] + (last,):
        await_blocks(2, k)
        for l in range(LAYERS):
            half_copy(l, DG, k).start()

    for k in range(KINDS):
        await_bytes(sent[k], d_send.at[k])
        await_bytes(p1[k], p1_send.at[k])
        await_bytes(p2[k], p2_send.at[k])
        await_bytes(got[k].at[pl.ds(0, LAYERS), pl.ds(0, 3)], g_send.at[k])
        await_bytes(got[k], h_send.at[k])
        await_bytes(got[k], h_recv.at[k])
    for which in range(6):
        await_bytes(all_ref.at[which, pl.ds(0, n_dev - 1)], ps_send.at[which])


def write_out(count, *refs):
    srcs, dsts, sems = refs[:count], refs[count:2 * count], refs[2 * count]
    copies = [pltpu.make_async_copy(src, dst, sems.at[i]) for i, (src, dst) in enumerate(zip(srcs, dsts))]
    for c in copies:
        c.start()
    for c in copies:
        c.wait()


def solution(mesh):
    n_model, n_data = mesh.shape["model"], mesh.shape["data"]
    in_specs = []
    for col_split in COLUMN_SPLIT:
        in_specs.extend([grad_spec(col_split), state_spec(col_split), state_spec(col_split), state_spec(col_split)])
    out_specs = tuple([replica_spec(col_split) for col_split in COLUMN_SPLIT] + [state_spec(col_split) for col_split in COLUMN_SPLIT] * 3)

    def device_step(*arrays):
        dims = [arrays[4 * k + 1].shape[1:] for k in range(KINDS)]
        f32, bf16 = jnp.float32, jnp.bfloat16
        out_shape = [jax.ShapeDtypeStruct((LAYERS, n_data * d[0], d[1]), bf16) for d in dims]
        out_shape += [jax.ShapeDtypeStruct((LAYERS,) + tuple(d), f32) for d in dims] * 3

        def each(prefix, dtype):
            return [pltpu.VMEM(prefix + tuple(d), dtype) for d in dims]

        dma = pltpu.SemaphoreType.DMA
        n_dev = n_model * n_data
        scratch = (each((LAYERS, 4), f32) + each((LAYERS,), f32) + each((LAYERS, 4), bf16) + each((LAYERS, 4), bf16)
                   + each((LAYERS, 2), f32) + each((LAYERS,), f32))
        scratch += [pltpu.VMEM((6, 1, 128), f32), pltpu.VMEM((6, n_dev, 1, 128), f32)]
        scratch += [dma((4, 2)), dma((4,)), dma((4,)), dma((4, 4)), dma((4,)), dma((2, 4)), dma((4,)), dma((4,)),
                    dma((4,)), dma((3, 4)), dma((4,)), dma((4,)), dma((6,)), dma((6,)), pltpu.SemaphoreType.REGULAR((n_model + 1,))]
        held = pl.pallas_call(
            functools.partial(kernel, n_model, n_data, dims),
            out_shape=[pltpu.VMEM(o.shape, o.dtype) for o in out_shape],
            in_specs=[pl.BlockSpec(memory_space=pl.ANY)] * 16,
            out_specs=[pl.BlockSpec(memory_space=pltpu.VMEM)] * 16,
            scratch_shapes=scratch,
            compiler_params=pltpu.CompilerParams(collective_id=0, has_side_effects=True, vmem_limit_bytes=COMM_VMEM),
            name="lamb_step",
        )(*arrays)
        held = [pltpu.with_memory_space_constraint(h, pltpu.VMEM) for h in held]
        return tuple(pl.pallas_call(
            functools.partial(write_out, len(out_shape)),
            out_shape=out_shape,
            in_specs=[pl.BlockSpec(memory_space=pltpu.VMEM)] * 16,
            out_specs=[pl.BlockSpec(memory_space=pl.ANY)] * 16,
            scratch_shapes=[dma((16,))],
            compiler_params=pltpu.CompilerParams(vmem_limit_bytes=1 << 20),
            name="write_out",
        )(*held))

    return jax.shard_map(device_step, mesh=mesh, in_specs=tuple(in_specs), out_specs=out_specs, check_vma=False)
```

```python
import functools

import jax
import jax.numpy as jnp
from jax import lax
from jax.experimental import pallas as pl
from jax.experimental.pallas import tpu as pltpu
from jax.sharding import PartitionSpec as P

LEARN_RATE = 0.08
BETA_ONE = 0.9
BETA_TWO = 0.999
ADAM_EPS = 1e-6
DECAY_RATE = 0.01
MAX_NORM = 1.0
STEP_COUNT = 100
COLUMN_SPLIT = (True, False, True, False)

KINDS = 4
LAYERS = 2
KIND_ORDER = (1, 0, 2, 3)
ME, XN, YN, DG = 0, 1, 2, 3
MESH = pl.DeviceIdType.MESH
COMM_VMEM = 42 << 20


def grad_spec(col_split):
    return P("data", None, None, "model") if col_split else P("data", None, "model", None)


def state_spec(col_split):
    return P(None, "data", "model") if col_split else P(None, ("model", "data"), None)


def replica_spec(col_split):
    return P(None, None, "model") if col_split else P(None, "model", None)


def lane_fold(x):
    total = x[:, 0:128]
    for j in range(1, x.shape[1] // 128):
        total = total + x[:, 128 * j:128 * (j + 1)]
    return total


def kernel(n_model, n_data, dims, *refs):
    n_dev = n_model * n_data
    grads, weights, firsts, seconds = ([refs[4 * k + i] for k in range(KINDS)] for i in range(4))
    outs = refs[16:32]
    replicas, wv, mv, vv = outs[0:4], outs[4:8], outs[8:12], outs[12:16]
    scratch = refs[32:]
    acc, stage, sent, got, p1, p2 = (scratch[4 * i:4 * i + 4] for i in range(6))
    (row_ref, all_ref, ld_unit, ld_state, d_send, d_recv, p1_send, p1_recv, p2_send, p2_recv,
     g_send, g_recv, h_send, h_recv, ps_send, ps_recv, raw_sem, rounds, raw_out, raw_in, raw_peer) = scratch[24:]

    model = lax.axis_index("model")
    data = lax.axis_index("data")
    core = data % 2
    xc = (data // 2) % 2
    yc = data // 4
    me = model * n_data + data

    def chip_of(slot):
        x = xc if slot in (ME, YN) else 1 - xc
        y = yc if slot in (ME, XN) else 1 - yc
        return 2 * y + x

    def device(slot, other_core=False):
        return (model, 2 * chip_of(slot) + ((1 - core) if other_core else core))

    partner = device(ME, True)
    to_x = device(XN)
    to_y = device(YN)

    def rows_of(k, slot, other_core):
        rows = dims[k][0]
        return pl.ds(pl.multiple_of((2 * chip_of(slot) + ((1 - core) if other_core else core)) * rows, rows), rows)

    def load_unit(l, s, k):
        pltpu.make_async_copy(grads[k].at[0, l, rows_of(k, s, True)], stage[k].at[l], ld_unit.at[k, l]).start()
        pltpu.make_async_copy(grads[k].at[0, l, rows_of(k, s, False)], acc[k].at[l, s], ld_unit.at[k, l]).start()

    def remote(src, dst, send, recv, dev):
        return pltpu.make_async_remote_copy(src_ref=src, dst_ref=dst, send_sem=send, recv_sem=recv, device_id=dev, device_id_type=MESH)

    def await_bytes(ref, sem):
        pltpu.make_async_copy(ref, ref, sem).wait()

    first_dev = (to_x, to_y)
    second_dev = (to_y, to_x)
    first_nb = (XN, YN)
    second_nb = (YN, XN)

    def over_rows(k, step, body):
        def run(i, carry):
            body(pl.ds(pl.multiple_of(i * step, step), step))
            return carry

        lax.fori_loop(0, dims[k][0] // step, run, 0)

    def sum_rows(k, body):
        rows, cols = dims[k]
        return lane_fold(lax.fori_loop(
            0, rows // 8, lambda i, c: c + body(pl.ds(pl.multiple_of(i * 8, 8), 8)), jnp.zeros((8, cols), jnp.float32)))

    pairs = [(slots, k) for slots in ((DG, DG), (YN, XN), (XN, YN), (ME, ME)) for k in KIND_ORDER]
    ahead = 3

    def load_pair(slots, k):
        for l in range(LAYERS):
            load_unit(l, slots[l], k)

    barrier = pltpu.get_barrier_semaphore()
    hops = 3 + jnp.minimum(model, 1) + jnp.minimum(n_model - 1 - model, 1)

    def greet(sem):
        for dev in (partner, to_x, to_y):
            pl.semaphore_signal(sem, inc=1, device_id=dev, device_id_type=MESH)

        @pl.when(model > 0)
        def _():
            pl.semaphore_signal(sem, inc=1, device_id=(model - 1, data), device_id_type=MESH)

        @pl.when(model < n_model - 1)
        def _():
            pl.semaphore_signal(sem, inc=1, device_id=(model + 1, data), device_id_type=MESH)

    greet(barrier)
    for p in pairs[:ahead]:
        load_pair(*p)

    first_kind = KIND_ORDER[0]
    later_kinds = KIND_ORDER[1:]

    def cast_rows(k, l, s):
        def body(r):
            sent[k][l, s, r, :] = stage[k][l, r, :].astype(jnp.bfloat16)

        over_rows(k, 16, body)

    def await_unit(k, l):
        await_bytes(acc[k].at[l, pl.ds(0, 2)], ld_unit.at[k, l])

    for l in range(LAYERS):
        await_unit(first_kind, l)

        def body(r):
            raw_out[l, 0, r, :] = acc[first_kind][l, DG, r, :].astype(jnp.bfloat16)
            raw_out[l, 1, r, :] = stage[first_kind][l, r, :].astype(jnp.bfloat16)

        over_rows(first_kind, 16, body)
    load_pair(*pairs[ahead])
    for l in range(LAYERS):
        await_unit(pairs[1][1], l)
        cast_rows(pairs[1][1], l, pairs[1][0][l])

    pl.semaphore_wait(barrier, hops)
    for l in range(LAYERS):
        remote(raw_out.at[l], raw_in.at[l], raw_sem.at[0], raw_sem.at[1], first_dev[l]).start()

    def pair_send(g, slots, k):
        for l in range(LAYERS):
            remote(sent[k].at[l, slots[l]], got[k].at[l, slots[l]], d_send.at[k], d_recv.at[g, k], partner).start()

    pair_send(0, *pairs[1])
    n_rounds = 2 + n_model - 1
    greet(rounds.at[0])

    def next_round(r):
        pl.semaphore_wait(rounds.at[r], hops)
        if r + 1 < n_rounds:
            greet(rounds.at[r + 1])

    def load_state(k):
        for src, dst in ((weights, wv), (firsts, mv), (seconds, vv)):
            pltpu.make_async_copy(src[k], dst[k], ld_state.at[k]).start()

    def pair_half(g, slots, k):
        for l in range(LAYERS):
            await_unit(k, l)
            cast_rows(k, l, slots[l])
        pair_send(g, slots, k)

    def chip_half(g, slots, k):
        await_bytes(got[k].at[pl.ds(0, LAYERS), 0], d_recv.at[g, k])
        for l in range(LAYERS):
            s = slots[l]

            def body(r):
                own = acc[k][l, s, r, :].astype(jnp.bfloat16).astype(jnp.float32)
                acc[k][l, s, r, :] = own + got[k][l, s, r, :].astype(jnp.float32)

            over_rows(k, 16, body)
            if s == DG or s == first_nb[l]:
                t = 0 if s == DG else 1
                remote(acc[k].at[l, s], p1[k].at[l, t], p1_send.at[k], p1_recv.at[t, k], first_dev[l]).start()

    for i in range(1, len(pairs) + 1):
        if i < len(pairs):
            if i >= 2:
                pair_half(i // KINDS, *pairs[i])
            if i + ahead < len(pairs):
                load_pair(*pairs[i + ahead])
            else:
                for k in (KIND_ORDER[i + ahead - len(pairs)],) + ((KIND_ORDER[ahead],) if i + 1 == len(pairs) else ()):
                    load_state(k)
        if i >= 2:
            chip_half((i - 1) // KINDS, *pairs[i - 1])
        if i >= 4 and i % 2 == 0 and (i - 4) // 2 < n_rounds:
            next_round((i - 4) // 2)

    await_bytes(raw_in, raw_sem.at[1])
    for l in range(LAYERS):
        remote(raw_in.at[l, 1], raw_peer.at[l], raw_sem.at[2], raw_sem.at[3], partner).start()
    for k in later_kinds + (first_kind,):
        if k == first_kind:
            await_bytes(raw_peer, raw_sem.at[3])
        else:
            await_bytes(p1[k].at[pl.ds(0, LAYERS), 0], p1_recv.at[0, k])
        for l in range(LAYERS):
            s = second_nb[l]

            def body(r):
                if k == first_kind:
                    come = raw_in[l, 0, r, :].astype(jnp.float32) + raw_peer[l, r, :].astype(jnp.float32)
                else:
                    come = p1[k][l, 0, r, :]
                acc[k][l, s, r, :] = acc[k][l, s, r, :] + come

            over_rows(k, 16, body)
            remote(acc[k].at[l, s], p2[k].at[l], p2_send.at[k], p2_recv.at[k], second_dev[l]).start()

    def share(which, row):
        row_ref[which] = row
        all_ref[which, me] = row
        for dz in sorted(range(n_model), key=lambda z: -min(z, n_model - z)):
            for dd in reversed(range(n_data)):
                if dz or dd:
                    remote(row_ref.at[which], all_ref.at[which, me], ps_send.at[which], ps_recv.at[which],
                           ((model + dz) % n_model, (data + dd) % n_data)).start()

    def shared(which):
        await_bytes(all_ref.at[which, pl.ds(0, n_dev - 1)], ps_recv.at[which])
        return jnp.sum(all_ref[which], axis=0)

    lane = lax.broadcasted_iota(jnp.int32, (1, 128), 1)

    def put(i, part):
        return jnp.where(lane == i, jnp.sum(part, keepdims=True), 0.0)

    def pick(row, i):
        return jnp.sum(jnp.where(lane == i, row, 0.0), axis=1, keepdims=True)

    norms = jnp.zeros((1, 128), jnp.float32)
    for k in KIND_ORDER:
        await_bytes(acc[k].at[pl.ds(0, LAYERS), pl.ds(0, 3)], ld_state.at[k])
        for l in range(LAYERS):
            norms = norms + put(2 * k + l, sum_rows(k, lambda r: wv[k][l, r, :] * wv[k][l, r, :]))

    for k in KIND_ORDER:
        await_bytes(p1[k].at[pl.ds(0, LAYERS), 0], p1_recv.at[1, k])
        for l in range(LAYERS):

            def body(r):
                acc[k][l, ME, r, :] = acc[k][l, ME, r, :] + p1[k][l, 1, r, :]

            over_rows(k, 8, body)

    grad_sq = jnp.zeros((8, 128), jnp.float32)
    for k in later_kinds + (first_kind,):
        await_bytes(p2[k], p2_recv.at[k])
        for l in range(LAYERS):

            def body(r):
                mean = (acc[k][l, ME, r, :] + p2[k][l, r, :]) * (1.0 / n_data)
                acc[k][l, ME, r, :] = mean
                return mean * mean

            grad_sq = grad_sq + sum_rows(k, body)
    share(4, jnp.sum(grad_sq, axis=0, keepdims=True))
    total_sq = jnp.sum(shared(4), axis=1, keepdims=True)
    clip = jnp.minimum(1.0, MAX_NORM / jnp.sqrt(total_sq))
    first_gain = (1.0 - BETA_ONE) * clip
    second_gain = (1.0 - BETA_TWO) * clip * clip
    root_scale = (1.0 - BETA_TWO ** STEP_COUNT) ** 0.5
    hat_scale = root_scale / (1.0 - BETA_ONE ** STEP_COUNT)

    for k in KIND_ORDER:
        squares = norms
        for l in range(LAYERS):

            def body(r):
                mean = acc[k][l, ME, r, :]
                first = BETA_ONE * mv[k][l, r, :] + first_gain * mean
                second = BETA_TWO * vv[k][l, r, :] + second_gain * (mean * mean)
                mv[k][l, r, :] = first
                vv[k][l, r, :] = second
                update = (hat_scale * first) / (jnp.sqrt(second) + ADAM_EPS * root_scale) + DECAY_RATE * wv[k][l, r, :]
                acc[k][l, ME, r, :] = update
                return update * update

            squares = squares + put(8 + 2 * k + l, sum_rows(k, body))
        share(k, squares)

    def block(l, s, k):
        return replicas[k].at[l, rows_of(k, s, False)]

    def own_copy(l, second, k):
        return remote(block(l, ME, k), block(l, ME, k), g_send.at[k], g_recv.at[second, k], second_dev[l] if second else first_dev[l])

    def pass_copy(l, k):
        src = block(l, first_nb[l], k)
        return remote(src, src, g_send.at[k], g_recv.at[2, k], second_dev[l])

    def half_copy(l, s, k):
        return remote(block(l, s, k), block(l, s, k), h_send.at[k], h_recv.at[k], partner)

    def await_blocks(i, k):
        await_bytes(got[k].at[pl.ds(0, LAYERS), 0], g_recv.at[i, k])

    for k in KIND_ORDER:
        roots = jnp.sqrt(shared(k))
        for l in range(LAYERS):
            scale = LEARN_RATE * (pick(roots, 2 * k + l) / pick(roots, 8 + 2 * k + l))
            start = pl.multiple_of(data * dims[k][0], dims[k][0])

            def body(r, at):
                fresh = wv[k][l, r, :] - scale * acc[k][l, ME, r, :]
                wv[k][l, r, :] = fresh
                replicas[k][l, pl.ds(pl.multiple_of(start + at, 16), 16), :] = fresh.astype(jnp.bfloat16)

            lax.fori_loop(0, dims[k][0] // 16, lambda i, c: (body(pl.ds(pl.multiple_of(i * 16, 16), 16), i * 16), c)[1], 0)
            own_copy(l, 0, k).start()
    for k in KIND_ORDER:
        for l in range(LAYERS):
            own_copy(l, 1, k).start()
            half_copy(l, ME, k).start()

    last = KIND_ORDER[0]
    for k in KIND_ORDER:
        await_blocks(0, k)
        for l in range(LAYERS):
            if k != last:
                pass_copy(l, k).start()
            half_copy(l, first_nb[l], k).start()
    for l in range(LAYERS):
        pass_copy(l, last).start()
    for k in KIND_ORDER:
        await_blocks(1, k)
        for l in range(LAYERS):
            half_copy(l, second_nb[l], k).start()
    for k in KIND_ORDER[1:] + (last,):
        await_blocks(2, k)
        for l in range(LAYERS):
            half_copy(l, DG, k).start()

    for k in range(KINDS):
        if k == first_kind:
            await_bytes(sent[k].at[pl.ds(0, LAYERS), pl.ds(0, 3)], d_send.at[k])
            await_bytes(p1[k].at[pl.ds(0, LAYERS), 1], p1_send.at[k])
        else:
            await_bytes(sent[k], d_send.at[k])
            await_bytes(p1[k], p1_send.at[k])
        await_bytes(p2[k], p2_send.at[k])
        await_bytes(got[k].at[pl.ds(0, LAYERS), pl.ds(0, 3)], g_send.at[k])
        await_bytes(got[k], h_send.at[k])
        await_bytes(got[k], h_recv.at[k])
    await_bytes(raw_in, raw_sem.at[0])
    await_bytes(raw_peer, raw_sem.at[2])
    for which in range(5):
        await_bytes(all_ref.at[which, pl.ds(0, n_dev - 1)], ps_send.at[which])


def write_out(count, *refs):
    srcs, dsts, sems = refs[:count], refs[count:2 * count], refs[2 * count]
    copies = [pltpu.make_async_copy(src, dst, sems.at[i]) for i, (src, dst) in enumerate(zip(srcs, dsts))]
    for c in copies:
        c.start()
    for c in copies:
        c.wait()


def solution(mesh):
    n_model, n_data = mesh.shape["model"], mesh.shape["data"]
    in_specs = []
    for col_split in COLUMN_SPLIT:
        in_specs.extend([grad_spec(col_split), state_spec(col_split), state_spec(col_split), state_spec(col_split)])
    out_specs = tuple([replica_spec(col_split) for col_split in COLUMN_SPLIT] + [state_spec(col_split) for col_split in COLUMN_SPLIT] * 3)

    def device_step(*arrays):
        dims = [arrays[4 * k + 1].shape[1:] for k in range(KINDS)]
        f32, bf16 = jnp.float32, jnp.bfloat16
        out_shape = [jax.ShapeDtypeStruct((LAYERS, n_data * d[0], d[1]), bf16) for d in dims]
        out_shape += [jax.ShapeDtypeStruct((LAYERS,) + tuple(d), f32) for d in dims] * 3

        def each(prefix, dtype):
            return [pltpu.VMEM(prefix + tuple(d), dtype) for d in dims]

        dma = pltpu.SemaphoreType.DMA
        n_dev = n_model * n_data
        scratch = (each((LAYERS, 4), f32) + each((LAYERS,), f32) + each((LAYERS, 4), bf16) + each((LAYERS, 4), bf16)
                   + each((LAYERS, 2), f32) + each((LAYERS,), f32))
        scratch += [pltpu.VMEM((5, 1, 128), f32), pltpu.VMEM((5, n_dev, 1, 128), f32)]
        scratch += [dma((4, 2)), dma((4,)), dma((4,)), dma((4, 4)), dma((4,)), dma((2, 4)), dma((4,)), dma((4,)),
                    dma((4,)), dma((3, 4)), dma((4,)), dma((4,)), dma((5,)), dma((5,)), dma((4,)), pltpu.SemaphoreType.REGULAR((n_model + 1,))]
        first = tuple(dims[KIND_ORDER[0]])
        scratch += [pltpu.VMEM((LAYERS, 2) + first, bf16), pltpu.VMEM((LAYERS, 2) + first, bf16), pltpu.VMEM((LAYERS,) + first, bf16)]
        held = pl.pallas_call(
            functools.partial(kernel, n_model, n_data, dims),
            out_shape=[pltpu.VMEM(o.shape, o.dtype) for o in out_shape],
            in_specs=[pl.BlockSpec(memory_space=pl.ANY)] * 16,
            out_specs=[pl.BlockSpec(memory_space=pltpu.VMEM)] * 16,
            scratch_shapes=scratch,
            compiler_params=pltpu.CompilerParams(collective_id=0, has_side_effects=True, vmem_limit_bytes=COMM_VMEM),
            name="lamb_step",
        )(*arrays)
        held = [pltpu.with_memory_space_constraint(h, pltpu.VMEM) for h in held]
        return tuple(pl.pallas_call(
            functools.partial(write_out, len(out_shape)),
            out_shape=out_shape,
            in_specs=[pl.BlockSpec(memory_space=pltpu.VMEM)] * 16,
            out_specs=[pl.BlockSpec(memory_space=pl.ANY)] * 16,
            scratch_shapes=[dma((16,))],
            compiler_params=pltpu.CompilerParams(vmem_limit_bytes=1 << 20),
            name="write_out",
        )(*held))

    return jax.shard_map(device_step, mesh=mesh, in_specs=tuple(in_specs), out_specs=out_specs, check_vma=False)
```

```python
import functools

import jax
import jax.numpy as jnp
from jax import lax
from jax.experimental import pallas as pl
from jax.experimental.pallas import tpu as pltpu
from jax.sharding import PartitionSpec as P

LEARN_RATE = 0.08
BETA_ONE = 0.9
BETA_TWO = 0.999
ADAM_EPS = 1e-6
DECAY_RATE = 0.01
MAX_NORM = 1.0
STEP_COUNT = 100
TINY = 1e-36
COLUMN_SPLIT = (True, False, True, False)

KINDS = 4
LAYERS = 2
KIND_ORDER = (1, 0, 2, 3)
NORM_GROUPS = ((1,), (0,), (2, 3))
GROUPS = len(NORM_GROUPS)
ME, XN, YN, DG = 0, 1, 2, 3
MESH = pl.DeviceIdType.MESH
COMM_VMEM = 42 << 20


def grad_spec(col_split):
    return P("data", None, None, "model") if col_split else P("data", None, "model", None)


def state_spec(col_split):
    return P(None, "data", "model") if col_split else P(None, ("model", "data"), None)


def replica_spec(col_split):
    return P(None, None, "model") if col_split else P(None, "model", None)


def lane_fold(x):
    total = x[:, 0:128]
    for j in range(1, x.shape[1] // 128):
        total = total + x[:, 128 * j:128 * (j + 1)]
    return total


def kernel(n_model, n_data, dims, *refs):
    n_dev = n_model * n_data
    grads, weights, firsts, seconds = ([refs[4 * k + i] for k in range(KINDS)] for i in range(4))
    outs = refs[16:32]
    replicas, wv, mv, vv = outs[0:4], outs[4:8], outs[8:12], outs[12:16]
    scratch = refs[32:]
    acc, stage, sent, got, p1, p2 = (scratch[4 * i:4 * i + 4] for i in range(6))
    (row_ref, all_ref, ld_unit, ld_state, d_send, d_recv, p1_send, p1_recv, p2_send, p2_recv,
     g_send, g_recv, h_send, h_recv, ps_send, ps_recv, raw_sem, early_sem, rounds,
     raw_out, raw_in, raw_peer, early_w, early_u) = scratch[24:]

    model = lax.axis_index("model")
    data = lax.axis_index("data")
    core = data % 2
    xc = (data // 2) % 2
    yc = data // 4
    me = model * n_data + data

    def chip_of(slot):
        x = xc if slot in (ME, YN) else 1 - xc
        y = yc if slot in (ME, XN) else 1 - yc
        return 2 * y + x

    def device(slot, other_core=False):
        return (model, 2 * chip_of(slot) + ((1 - core) if other_core else core))

    partner = device(ME, True)
    to_x = device(XN)
    to_y = device(YN)

    def rows_of(k, slot, other_core):
        rows = dims[k][0]
        return pl.ds(pl.multiple_of((2 * chip_of(slot) + ((1 - core) if other_core else core)) * rows, rows), rows)

    def load_unit(l, s, k):
        pltpu.make_async_copy(grads[k].at[0, l, rows_of(k, s, True)], stage[k].at[l], ld_unit.at[k, l]).start()
        pltpu.make_async_copy(grads[k].at[0, l, rows_of(k, s, False)], acc[k].at[l, s], ld_unit.at[k, l]).start()

    def remote(src, dst, send, recv, dev):
        return pltpu.make_async_remote_copy(src_ref=src, dst_ref=dst, send_sem=send, recv_sem=recv, device_id=dev, device_id_type=MESH)

    def await_bytes(ref, sem):
        pltpu.make_async_copy(ref, ref, sem).wait()

    first_dev = (to_x, to_y)
    second_dev = (to_y, to_x)
    first_nb = (XN, YN)
    second_nb = (YN, XN)

    def over_rows(k, step, body):
        def run(i, carry):
            body(pl.ds(pl.multiple_of(i * step, step), step))
            return carry

        lax.fori_loop(0, dims[k][0] // step, run, 0)

    def sum_rows(k, body):
        rows, cols = dims[k]

        def run(i, carry):
            r = pl.ds(pl.multiple_of(i * 8, 8), 8)
            return tuple(carry[l] + body(l, r) for l in range(LAYERS))

        sums = lax.fori_loop(0, rows // 8, run, (jnp.zeros((8, cols), jnp.float32),) * LAYERS)
        return [lane_fold(x) for x in sums]

    pairs = [(slots, k) for slots in ((DG, DG), (YN, XN), (XN, YN), (ME, ME)) for k in KIND_ORDER]
    ahead = 3

    def load_pair(slots, k):
        for l in range(LAYERS):
            load_unit(l, slots[l], k)

    barrier = pltpu.get_barrier_semaphore()
    z_hops = jnp.minimum(model, 1) + jnp.minimum(n_model - 1 - model, 1)

    def greet_z(sem):
        @pl.when(model > 0)
        def _():
            pl.semaphore_signal(sem, inc=1, device_id=(model - 1, data), device_id_type=MESH)

        @pl.when(model < n_model - 1)
        def _():
            pl.semaphore_signal(sem, inc=1, device_id=(model + 1, data), device_id_type=MESH)

    for dev in (partner, to_x, to_y):
        pl.semaphore_signal(barrier, inc=1, device_id=dev, device_id_type=MESH)
    greet_z(barrier)
    for p in pairs[:ahead]:
        load_pair(*p)

    first_kind = KIND_ORDER[0]
    later_kinds = KIND_ORDER[1:]

    def cast_rows(k, l, s):
        def body(r):
            sent[k][l, s, r, :] = stage[k][l, r, :].astype(jnp.bfloat16)

        over_rows(k, 16, body)

    def await_unit(k, l):
        await_bytes(acc[k].at[l, pl.ds(0, 2)], ld_unit.at[k, l])

    for l in range(LAYERS):
        await_unit(first_kind, l)

        def body(r):
            raw_out[l, 0, r, :] = acc[first_kind][l, DG, r, :].astype(jnp.bfloat16)
            raw_out[l, 1, r, :] = stage[first_kind][l, r, :].astype(jnp.bfloat16)

        over_rows(first_kind, 16, body)
    load_pair(*pairs[ahead])
    for l in range(LAYERS):
        await_unit(pairs[1][1], l)
        cast_rows(pairs[1][1], l, pairs[1][0][l])

    pl.semaphore_wait(barrier, 3 + z_hops)
    for l in range(LAYERS):
        remote(raw_out.at[l], raw_in.at[l], raw_sem.at[0], raw_sem.at[1], first_dev[l]).start()

    def pair_send(g, slots, k):
        for l in range(LAYERS):
            remote(sent[k].at[l, slots[l]], got[k].at[l, slots[l]], d_send.at[k], d_recv.at[g, k], partner).start()

    pair_send(0, *pairs[1])
    axes = ("z",) * (n_model - 2) + ("core", "x", "y")
    n_rounds = len(axes)

    def greet_round(r):
        if axes[r] == "z":
            greet_z(rounds.at[r])
        else:
            pl.semaphore_signal(rounds.at[r], inc=1, device_id={"core": partner, "x": to_x, "y": to_y}[axes[r]], device_id_type=MESH)

    greet_round(0)

    def next_round(r):
        pl.semaphore_wait(rounds.at[r], z_hops if axes[r] == "z" else 1)
        if r + 1 < n_rounds:
            greet_round(r + 1)

    def load_state(k):
        for src, dst in ((weights, wv), (firsts, mv), (seconds, vv)):
            pltpu.make_async_copy(src[k], dst[k], ld_state.at[k]).start()

    def pair_half(g, slots, k):
        for l in range(LAYERS):
            await_unit(k, l)
            cast_rows(k, l, slots[l])
        pair_send(g, slots, k)

    def chip_half(g, slots, k):
        await_bytes(got[k].at[pl.ds(0, LAYERS), 0], d_recv.at[g, k])
        for l in range(LAYERS):
            s = slots[l]

            def body(r):
                own = acc[k][l, s, r, :].astype(jnp.bfloat16).astype(jnp.float32)
                acc[k][l, s, r, :] = own + got[k][l, s, r, :].astype(jnp.float32)

            over_rows(k, 16, body)
            if s == DG or s == first_nb[l]:
                t = 0 if s == DG else 1
                remote(acc[k].at[l, s], p1[k].at[l, t], p1_send.at[k], p1_recv.at[t, k], first_dev[l]).start()

    for i in range(1, len(pairs) + 1):
        if i < len(pairs):
            if i >= 2:
                pair_half(i // KINDS, *pairs[i])
            if i + ahead < len(pairs):
                load_pair(*pairs[i + ahead])
            else:
                for k in (KIND_ORDER[i + ahead - len(pairs)],) + ((KIND_ORDER[ahead],) if i + 1 == len(pairs) else ()):
                    load_state(k)
        if i >= 2:
            chip_half((i - 1) // KINDS, *pairs[i - 1])
        if i >= 4 and i % 2 == 0 and (i - 4) // 2 < n_rounds:
            next_round((i - 4) // 2)

    await_bytes(raw_in, raw_sem.at[1])
    for l in range(LAYERS):
        remote(raw_in.at[l, 1], raw_peer.at[l], raw_sem.at[2], raw_sem.at[3], partner).start()
    for k in later_kinds + (first_kind,):
        if k == first_kind:
            await_bytes(raw_peer, raw_sem.at[3])
        else:
            await_bytes(p1[k].at[pl.ds(0, LAYERS), 0], p1_recv.at[0, k])
        for l in range(LAYERS):
            s = second_nb[l]

            def body(r):
                if k == first_kind:
                    come = raw_in[l, 0, r, :].astype(jnp.float32) + raw_peer[l, r, :].astype(jnp.float32)
                else:
                    come = p1[k][l, 0, r, :]
                acc[k][l, s, r, :] = acc[k][l, s, r, :] + come

            over_rows(k, 16, body)
            remote(acc[k].at[l, s], p2[k].at[l], p2_send.at[k], p2_recv.at[k], second_dev[l]).start()

    def share(which, row):
        row_ref[which] = row
        all_ref[which, me] = row
        for dz in sorted(range(n_model), key=lambda z: -min(z, n_model - z)):
            for dd in reversed(range(n_data)):
                if dz or dd:
                    remote(row_ref.at[which], all_ref.at[which, me], ps_send.at[which], ps_recv.at[which],
                           ((model + dz) % n_model, (data + dd) % n_data)).start()

    def shared(which):
        await_bytes(all_ref.at[which, pl.ds(0, n_dev - 1)], ps_recv.at[which])
        return jnp.sum(all_ref[which], axis=0)

    lane = lax.broadcasted_iota(jnp.int32, (1, 128), 1)

    def put(i, part):
        return jnp.where(lane == i, jnp.sum(part, keepdims=True), 0.0)

    def pick(row, i):
        return jnp.sum(jnp.where(lane == i, row, 0.0), axis=1, keepdims=True)

    norms = jnp.zeros((1, 128), jnp.float32)
    for k in KIND_ORDER:
        await_bytes(acc[k].at[pl.ds(0, LAYERS), pl.ds(0, 3)], ld_state.at[k])
        for l, part in enumerate(sum_rows(k, lambda l, r: wv[k][l, r, :] * wv[k][l, r, :])):
            norms = norms + put(2 * k + l, part)

    for k in KIND_ORDER:
        await_bytes(p1[k].at[pl.ds(0, LAYERS), 0], p1_recv.at[1, k])
        for l in range(LAYERS):

            def body(r):
                acc[k][l, ME, r, :] = acc[k][l, ME, r, :] + p1[k][l, 1, r, :]

            over_rows(k, 8, body)

    grad_sq = jnp.zeros((8, 128), jnp.float32)
    for k in later_kinds + (first_kind,):
        await_bytes(p2[k], p2_recv.at[k])

        def body(l, r):
            mean = (acc[k][l, ME, r, :] + p2[k][l, r, :]) * (1.0 / n_data)
            acc[k][l, ME, r, :] = mean
            return mean * mean

        for part in sum_rows(k, body):
            grad_sq = grad_sq + part
    share(GROUPS, jnp.sum(grad_sq, axis=0, keepdims=True))

    for l in range(LAYERS):
        remote(wv[first_kind].at[l], early_w.at[l], early_sem.at[0], early_sem.at[1], first_dev[l]).start()
    total_sq = jnp.sum(shared(GROUPS), axis=1, keepdims=True)
    clip = jnp.minimum(1.0, MAX_NORM / jnp.sqrt(total_sq))
    first_gain = (1.0 - BETA_ONE) * clip
    second_gain = (1.0 - BETA_TWO) * clip * clip
    root_scale = (1.0 - BETA_TWO ** STEP_COUNT) ** 0.5
    hat_scale = root_scale / (1.0 - BETA_ONE ** STEP_COUNT)

    def updates(k):
        def body(l, r):
            mean = acc[k][l, ME, r, :]
            first = BETA_ONE * mv[k][l, r, :] + first_gain * mean
            second = BETA_TWO * vv[k][l, r, :] + second_gain * (mean * mean)
            mv[k][l, r, :] = first
            vv[k][l, r, :] = second
            root = jnp.maximum(second, TINY)
            root = root * lax.rsqrt(root)
            update = (hat_scale * first) / (root + ADAM_EPS * root_scale) + DECAY_RATE * wv[k][l, r, :]
            acc[k][l, ME, r, :] = update
            return update * update

        return sum_rows(k, body)

    for g, kinds in enumerate(NORM_GROUPS):
        squares = norms
        for k in kinds:
            for l, part in enumerate(updates(k)):
                squares = squares + put(8 + 2 * k + l, part)
        share(g, squares)
        if g < 2:
            half = dims[first_kind][0] // 2
            piece = pl.ds(g * half, half)
            for l in range(LAYERS):
                remote(acc[first_kind].at[l, ME, piece], early_u.at[l, piece], early_sem.at[2], early_sem.at[3], first_dev[l]).start()

    def block(l, s, k):
        return replicas[k].at[l, rows_of(k, s, False)]

    def own_copy(l, second, k):
        return remote(block(l, ME, k), block(l, ME, k), g_send.at[k], g_recv.at[second, k], second_dev[l] if second else first_dev[l])

    def pass_copy(l, k):
        src = block(l, first_nb[l], k)
        return remote(src, src, g_send.at[k], g_recv.at[2, k], second_dev[l])

    def half_copy(l, s, k):
        return remote(block(l, s, k), block(l, s, k), h_send.at[k], h_recv.at[k], partner)

    def await_blocks(i, k):
        await_bytes(got[k].at[pl.ds(0, LAYERS), 0], g_recv.at[i, k])

    def new_rows(k, l, s, scale, take):
        start = pl.multiple_of((2 * chip_of(s) + core) * dims[k][0], dims[k][0])

        def run(i, carry):
            at = i * 16
            replicas[k][l, pl.ds(pl.multiple_of(start + at, 16), 16), :] = take(pl.ds(pl.multiple_of(at, 16), 16), scale).astype(jnp.bfloat16)
            return carry

        lax.fori_loop(0, dims[k][0] // 16, run, 0)

    for g, kinds in enumerate(NORM_GROUPS):
        roots = jnp.sqrt(shared(g))
        scales = {(k, l): LEARN_RATE * (pick(roots, 2 * k + l) / pick(roots, 8 + 2 * k + l)) for k in kinds for l in range(LAYERS)}
        if g == 0:
            await_bytes(early_w, early_sem.at[0])
        for k in kinds:
            for l in range(LAYERS):

                def fresh_rows(r, scale):
                    fresh = wv[k][l, r, :] - scale * acc[k][l, ME, r, :]
                    wv[k][l, r, :] = fresh
                    return fresh

                new_rows(k, l, ME, scales[k, l], fresh_rows)
                own_copy(l, 1 if g == 0 else 0, k).start()
        if g == 0:
            first_scales = scales
            for l in range(LAYERS):
                half_copy(l, ME, first_kind).start()

    for k in later_kinds:
        for l in range(LAYERS):
            own_copy(l, 1, k).start()
            half_copy(l, ME, k).start()

    await_bytes(early_w, early_sem.at[1])
    await_bytes(early_u, early_sem.at[3])
    for l in range(LAYERS):
        new_rows(first_kind, l, first_nb[l], first_scales[first_kind, l], lambda r, scale: early_w[l, r, :] - scale * early_u[l, r, :])
        half_copy(l, first_nb[l], first_kind).start()
    for k in later_kinds:
        await_blocks(0, k)
        for l in range(LAYERS):
            pass_copy(l, k).start()
            half_copy(l, first_nb[l], k).start()
    for l in range(LAYERS):
        pass_copy(l, first_kind).start()
    for k in KIND_ORDER:
        await_blocks(1, k)
        for l in range(LAYERS):
            half_copy(l, second_nb[l], k).start()
    for k in later_kinds + (first_kind,):
        await_blocks(2, k)
        for l in range(LAYERS):
            half_copy(l, DG, k).start()

    for k in range(KINDS):
        if k == first_kind:
            await_bytes(sent[k].at[pl.ds(0, LAYERS), pl.ds(0, 3)], d_send.at[k])
            await_bytes(p1[k].at[pl.ds(0, LAYERS), 1], p1_send.at[k])
        else:
            await_bytes(sent[k], d_send.at[k])
            await_bytes(p1[k], p1_send.at[k])
        await_bytes(p2[k], p2_send.at[k])
        await_bytes(got[k].at[pl.ds(0, LAYERS), pl.ds(0, 2 if k == first_kind else 3)], g_send.at[k])
        await_bytes(got[k], h_send.at[k])
        await_bytes(got[k], h_recv.at[k])
    await_bytes(raw_in, raw_sem.at[0])
    await_bytes(raw_peer, raw_sem.at[2])
    await_bytes(early_u, early_sem.at[2])
    for which in range(GROUPS + 1):
        await_bytes(all_ref.at[which, pl.ds(0, n_dev - 1)], ps_send.at[which])


def write_out(count, *refs):
    srcs, dsts, sems = refs[:count], refs[count:2 * count], refs[2 * count]
    copies = [pltpu.make_async_copy(src, dst, sems.at[i]) for i, (src, dst) in enumerate(zip(srcs, dsts))]
    for c in copies:
        c.start()
    for c in copies:
        c.wait()


def solution(mesh):
    n_model, n_data = mesh.shape["model"], mesh.shape["data"]
    in_specs = []
    for col_split in COLUMN_SPLIT:
        in_specs.extend([grad_spec(col_split), state_spec(col_split), state_spec(col_split), state_spec(col_split)])
    out_specs = tuple([replica_spec(col_split) for col_split in COLUMN_SPLIT] + [state_spec(col_split) for col_split in COLUMN_SPLIT] * 3)

    def device_step(*arrays):
        dims = [arrays[4 * k + 1].shape[1:] for k in range(KINDS)]
        f32, bf16 = jnp.float32, jnp.bfloat16
        out_shape = [jax.ShapeDtypeStruct((LAYERS, n_data * d[0], d[1]), bf16) for d in dims]
        out_shape += [jax.ShapeDtypeStruct((LAYERS,) + tuple(d), f32) for d in dims] * 3

        def each(prefix, dtype):
            return [pltpu.VMEM(prefix + tuple(d), dtype) for d in dims]

        dma = pltpu.SemaphoreType.DMA
        n_dev = n_model * n_data
        scratch = (each((LAYERS, 4), f32) + each((LAYERS,), f32) + each((LAYERS, 4), bf16) + each((LAYERS, 4), bf16)
                   + each((LAYERS, 2), f32) + each((LAYERS,), f32))
        scratch += [pltpu.VMEM((GROUPS + 1, 1, 128), f32), pltpu.VMEM((GROUPS + 1, n_dev, 1, 128), f32)]
        scratch += [dma((4, 2)), dma((4,)), dma((4,)), dma((4, 4)), dma((4,)), dma((2, 4)), dma((4,)), dma((4,)),
                    dma((4,)), dma((3, 4)), dma((4,)), dma((4,)), dma((GROUPS + 1,)), dma((GROUPS + 1,)), dma((4,)), dma((4,)), pltpu.SemaphoreType.REGULAR((n_model + 1,))]
        first = tuple(dims[KIND_ORDER[0]])
        scratch += [pltpu.VMEM((LAYERS, 2) + first, bf16), pltpu.VMEM((LAYERS, 2) + first, bf16), pltpu.VMEM((LAYERS,) + first, bf16)]
        scratch += [pltpu.VMEM((LAYERS,) + first, f32)] * 2
        held = pl.pallas_call(
            functools.partial(kernel, n_model, n_data, dims),
            out_shape=[pltpu.VMEM(o.shape, o.dtype) for o in out_shape],
            in_specs=[pl.BlockSpec(memory_space=pl.ANY)] * 16,
            out_specs=[pl.BlockSpec(memory_space=pltpu.VMEM)] * 16,
            scratch_shapes=scratch,
            compiler_params=pltpu.CompilerParams(collective_id=0, has_side_effects=True, vmem_limit_bytes=COMM_VMEM),
            name="lamb_step",
        )(*arrays)
        held = [pltpu.with_memory_space_constraint(h, pltpu.VMEM) for h in held]
        return tuple(pl.pallas_call(
            functools.partial(write_out, len(out_shape)),
            out_shape=out_shape,
            in_specs=[pl.BlockSpec(memory_space=pltpu.VMEM)] * 16,
            out_specs=[pl.BlockSpec(memory_space=pl.ANY)] * 16,
            scratch_shapes=[dma((16,))],
            compiler_params=pltpu.CompilerParams(vmem_limit_bytes=1 << 20),
            name="write_out",
        )(*held))

    return jax.shard_map(device_step, mesh=mesh, in_specs=tuple(in_specs), out_specs=out_specs, check_vma=False)
```

```python
import functools

import jax
import jax.numpy as jnp
from jax import lax
from jax.experimental import pallas as pl
from jax.experimental.pallas import tpu as pltpu
from jax.sharding import PartitionSpec as P

LEARN_RATE = 0.08
BETA_ONE = 0.9
BETA_TWO = 0.999
ADAM_EPS = 1e-6
DECAY_RATE = 0.01
MAX_NORM = 1.0
STEP_COUNT = 100
TINY = 1e-36
COLUMN_SPLIT = (True, False, True, False)

KINDS = 4
LAYERS = 2
KIND_ORDER = (1, 0, 2, 3)
NORM_GROUPS = ((1,), (0,), (2, 3))
GROUPS = len(NORM_GROUPS)
ME, XN, YN, DG = 0, 1, 2, 3
MESH = pl.DeviceIdType.MESH
COMM_VMEM = 42 << 20


def grad_spec(col_split):
    return P("data", None, None, "model") if col_split else P("data", None, "model", None)


def state_spec(col_split):
    return P(None, "data", "model") if col_split else P(None, ("model", "data"), None)


def replica_spec(col_split):
    return P(None, None, "model") if col_split else P(None, "model", None)


def lane_fold(x):
    total = x[:, 0:128]
    for j in range(1, x.shape[1] // 128):
        total = total + x[:, 128 * j:128 * (j + 1)]
    return total


def kernel(n_model, n_data, dims, *refs):
    n_dev = n_model * n_data
    grads, weights, firsts, seconds = ([refs[4 * k + i] for k in range(KINDS)] for i in range(4))
    outs = refs[16:32]
    replicas, wv, mv, vv = outs[0:4], outs[4:8], outs[8:12], outs[12:16]
    scratch = refs[32:]
    acc, stage, sent, got, p1, p2 = (scratch[4 * i:4 * i + 4] for i in range(6))
    (row_ref, all_ref, ld_unit, ld_state, d_send, d_recv, p1_send, p1_recv, p2_send, p2_recv,
     g_send, g_recv, h_send, h_recv, ps_send, ps_recv, raw_sem, early_sem, tail_sem, rounds,
     raw_out, raw_in, raw_peer, early_w, early_u) = scratch[24:]

    model = lax.axis_index("model")
    data = lax.axis_index("data")
    core = data % 2
    xc = (data // 2) % 2
    yc = data // 4
    me = model * n_data + data

    def chip_of(slot):
        x = xc if slot in (ME, YN) else 1 - xc
        y = yc if slot in (ME, XN) else 1 - yc
        return 2 * y + x

    def device(slot, other_core=False):
        return (model, 2 * chip_of(slot) + ((1 - core) if other_core else core))

    partner = device(ME, True)
    to_x = device(XN)
    to_y = device(YN)

    def rows_of(k, slot, other_core):
        rows = dims[k][0]
        return pl.ds(pl.multiple_of((2 * chip_of(slot) + ((1 - core) if other_core else core)) * rows, rows), rows)

    def load_unit(l, s, k):
        pltpu.make_async_copy(grads[k].at[0, l, rows_of(k, s, True)], stage[k].at[l], ld_unit.at[k, l]).start()
        pltpu.make_async_copy(grads[k].at[0, l, rows_of(k, s, False)], acc[k].at[l, s], ld_unit.at[k, l]).start()

    def remote(src, dst, send, recv, dev):
        return pltpu.make_async_remote_copy(src_ref=src, dst_ref=dst, send_sem=send, recv_sem=recv, device_id=dev, device_id_type=MESH)

    def await_bytes(ref, sem):
        pltpu.make_async_copy(ref, ref, sem).wait()

    first_dev = (to_x, to_y)
    second_dev = (to_y, to_x)
    first_nb = (XN, YN)
    second_nb = (YN, XN)

    def over_rows(k, step, body):
        def run(i, carry):
            body(pl.ds(pl.multiple_of(i * step, step), step))
            return carry

        lax.fori_loop(0, dims[k][0] // step, run, 0)

    def sum_rows(k, body):
        rows, cols = dims[k]

        def run(i, carry):
            r = pl.ds(pl.multiple_of(i * 8, 8), 8)
            return tuple(carry[l] + body(l, r) for l in range(LAYERS))

        sums = lax.fori_loop(0, rows // 8, run, (jnp.zeros((8, cols), jnp.float32),) * LAYERS)
        return [lane_fold(x) for x in sums]

    pairs = [(slots, k) for slots in ((DG, DG), (YN, XN), (XN, YN), (ME, ME)) for k in KIND_ORDER]
    ahead = 3

    def load_pair(slots, k):
        for l in range(LAYERS):
            load_unit(l, slots[l], k)

    barrier = pltpu.get_barrier_semaphore()
    z_hops = jnp.minimum(model, 1) + jnp.minimum(n_model - 1 - model, 1)

    def greet_z(sem):
        @pl.when(model > 0)
        def _():
            pl.semaphore_signal(sem, inc=1, device_id=(model - 1, data), device_id_type=MESH)

        @pl.when(model < n_model - 1)
        def _():
            pl.semaphore_signal(sem, inc=1, device_id=(model + 1, data), device_id_type=MESH)

    for dev in (partner, to_x, to_y):
        pl.semaphore_signal(barrier, inc=1, device_id=dev, device_id_type=MESH)
    greet_z(barrier)
    for p in pairs[:ahead]:
        load_pair(*p)

    first_kind = KIND_ORDER[0]
    later_kinds = KIND_ORDER[1:]

    def cast_rows(k, l, s):
        def body(r):
            sent[k][l, s, r, :] = stage[k][l, r, :].astype(jnp.bfloat16)

        over_rows(k, 16, body)

    def await_unit(k, l):
        await_bytes(acc[k].at[l, pl.ds(0, 2)], ld_unit.at[k, l])

    for l in range(LAYERS):
        await_unit(first_kind, l)

        def body(r):
            raw_out[l, 0, r, :] = acc[first_kind][l, DG, r, :].astype(jnp.bfloat16)
            raw_out[l, 1, r, :] = stage[first_kind][l, r, :].astype(jnp.bfloat16)

        over_rows(first_kind, 16, body)
    load_pair(*pairs[ahead])
    for l in range(LAYERS):
        await_unit(pairs[1][1], l)
        cast_rows(pairs[1][1], l, pairs[1][0][l])

    pl.semaphore_wait(barrier, 3 + z_hops)
    for l in range(LAYERS):
        remote(raw_out.at[l], raw_in.at[l], raw_sem.at[0], raw_sem.at[1], first_dev[l]).start()

    def pair_send(g, slots, k):
        for l in range(LAYERS):
            remote(sent[k].at[l, slots[l]], got[k].at[l, slots[l]], d_send.at[k], d_recv.at[g, k], partner).start()

    pair_send(0, *pairs[1])
    axes = ("z",) * (n_model - 2) + ("core", "x", "y")
    n_rounds = len(axes)

    def greet_round(r):
        if axes[r] == "z":
            greet_z(rounds.at[r])
        else:
            pl.semaphore_signal(rounds.at[r], inc=1, device_id={"core": partner, "x": to_x, "y": to_y}[axes[r]], device_id_type=MESH)

    greet_round(0)

    def next_round(r):
        pl.semaphore_wait(rounds.at[r], z_hops if axes[r] == "z" else 1)
        if r + 1 < n_rounds:
            greet_round(r + 1)

    def load_state(k):
        for src, dst in ((weights, wv), (firsts, mv), (seconds, vv)):
            pltpu.make_async_copy(src[k], dst[k], ld_state.at[k]).start()

    def pair_half(g, slots, k):
        for l in range(LAYERS):
            await_unit(k, l)
            cast_rows(k, l, slots[l])
        pair_send(g, slots, k)

    def chip_half(g, slots, k):
        await_bytes(got[k].at[pl.ds(0, LAYERS), 0], d_recv.at[g, k])
        for l in range(LAYERS):
            s = slots[l]

            def body(r):
                own = acc[k][l, s, r, :].astype(jnp.bfloat16).astype(jnp.float32)
                acc[k][l, s, r, :] = own + got[k][l, s, r, :].astype(jnp.float32)

            over_rows(k, 16, body)
            if s == DG or s == first_nb[l]:
                t = 0 if s == DG else 1
                remote(acc[k].at[l, s], p1[k].at[l, t], p1_send.at[k], p1_recv.at[t, k], first_dev[l]).start()

    for i in range(1, len(pairs) + 1):
        if i < len(pairs):
            if i >= 2:
                pair_half(i // KINDS, *pairs[i])
            if i + ahead < len(pairs):
                load_pair(*pairs[i + ahead])
            else:
                for k in (KIND_ORDER[i + ahead - len(pairs)],) + ((KIND_ORDER[ahead],) if i + 1 == len(pairs) else ()):
                    load_state(k)
        if i >= 2:
            chip_half((i - 1) // KINDS, *pairs[i - 1])
        if i >= 4 and i % 2 == 0 and (i - 4) // 2 < n_rounds:
            next_round((i - 4) // 2)

    await_bytes(raw_in, raw_sem.at[1])
    for l in range(LAYERS):
        remote(raw_in.at[l, 1], raw_peer.at[l], raw_sem.at[2], raw_sem.at[3], partner).start()
    for k in later_kinds + (first_kind,):
        if k == first_kind:
            await_bytes(raw_peer, raw_sem.at[3])
        else:
            await_bytes(p1[k].at[pl.ds(0, LAYERS), 0], p1_recv.at[0, k])
        for l in range(LAYERS):
            s = second_nb[l]

            def body(r):
                if k == first_kind:
                    come = raw_in[l, 0, r, :].astype(jnp.float32) + raw_peer[l, r, :].astype(jnp.float32)
                else:
                    come = p1[k][l, 0, r, :]
                acc[k][l, s, r, :] = acc[k][l, s, r, :] + come

            over_rows(k, 16, body)
            remote(acc[k].at[l, s], p2[k].at[l], p2_send.at[k], p2_recv.at[k], second_dev[l]).start()

    def share(which, row):
        row_ref[which] = row
        all_ref[which, me] = row
        for dz in sorted(range(n_model), key=lambda z: -min(z, n_model - z)):
            for dd in reversed(range(n_data)):
                if dz or dd:
                    remote(row_ref.at[which], all_ref.at[which, me], ps_send.at[0], ps_recv.at[which],
                           ((model + dz) % n_model, (data + dd) % n_data)).start()

    def shared(which):
        await_bytes(all_ref.at[which, pl.ds(0, n_dev - 1)], ps_recv.at[which])
        return jnp.sum(all_ref[which], axis=0)

    lane = lax.broadcasted_iota(jnp.int32, (1, 128), 1)

    def put(i, part):
        return jnp.where(lane == i, jnp.sum(part, keepdims=True), 0.0)

    def pick(row, i):
        return jnp.sum(jnp.where(lane == i, row, 0.0), axis=1, keepdims=True)

    norms = jnp.zeros((1, 128), jnp.float32)
    for k in KIND_ORDER:
        await_bytes(acc[k].at[pl.ds(0, LAYERS), pl.ds(0, 3)], ld_state.at[k])
        for l, part in enumerate(sum_rows(k, lambda l, r: wv[k][l, r, :] * wv[k][l, r, :])):
            norms = norms + put(2 * k + l, part)

    for k in KIND_ORDER:
        await_bytes(p1[k].at[pl.ds(0, LAYERS), 0], p1_recv.at[1, k])
        for l in range(LAYERS):

            def body(r):
                acc[k][l, ME, r, :] = acc[k][l, ME, r, :] + p1[k][l, 1, r, :]

            over_rows(k, 8, body)

    grad_sq = jnp.zeros((8, 128), jnp.float32)
    for k in later_kinds + (first_kind,):
        await_bytes(p2[k], p2_recv.at[k])

        def body(l, r):
            mean = (acc[k][l, ME, r, :] + p2[k][l, r, :]) * (1.0 / n_data)
            acc[k][l, ME, r, :] = mean
            return mean * mean

        for part in sum_rows(k, body):
            grad_sq = grad_sq + part
    share(GROUPS, jnp.sum(grad_sq, axis=0, keepdims=True))

    for l in range(LAYERS):
        remote(wv[first_kind].at[l], early_w.at[l], early_sem.at[0], early_sem.at[1], first_dev[l]).start()
    total_sq = jnp.sum(shared(GROUPS), axis=1, keepdims=True)
    clip = jnp.minimum(1.0, MAX_NORM / jnp.sqrt(total_sq))
    first_gain = (1.0 - BETA_ONE) * clip
    second_gain = (1.0 - BETA_TWO) * clip * clip
    root_scale = (1.0 - BETA_TWO ** STEP_COUNT) ** 0.5
    hat_scale = root_scale / (1.0 - BETA_ONE ** STEP_COUNT)

    def updates(k):
        def body(l, r):
            mean = acc[k][l, ME, r, :]
            first = BETA_ONE * mv[k][l, r, :] + first_gain * mean
            second = BETA_TWO * vv[k][l, r, :] + second_gain * (mean * mean)
            mv[k][l, r, :] = first
            vv[k][l, r, :] = second
            root = jnp.maximum(second, TINY)
            root = root * lax.rsqrt(root)
            update = (hat_scale * first) / (root + ADAM_EPS * root_scale) + DECAY_RATE * wv[k][l, r, :]
            acc[k][l, ME, r, :] = update
            return update * update

        return sum_rows(k, body)

    for g, kinds in enumerate(NORM_GROUPS):
        squares = norms
        for k in kinds:
            for l, part in enumerate(updates(k)):
                squares = squares + put(8 + 2 * k + l, part)
        share(g, squares)
        if g < 2:
            half = dims[first_kind][0] // 2
            piece = pl.ds(g * half, half)
            for l in range(LAYERS):
                remote(acc[first_kind].at[l, ME, piece], early_u.at[l, piece], early_sem.at[2], early_sem.at[3], first_dev[l]).start()

    def block(l, s, k):
        return replicas[k].at[l, rows_of(k, s, False)]

    def own_copy(l, second, k):
        return remote(block(l, ME, k), block(l, ME, k), g_send.at[k], g_recv.at[second, k], second_dev[l] if second else first_dev[l])

    def pass_copy(l, k):
        src = block(l, first_nb[l], k)
        return remote(src, src, g_send.at[k], g_recv.at[2, k], second_dev[l])

    def half_copy(l, s, k):
        return remote(block(l, s, k), block(l, s, k), h_send.at[k], h_recv.at[k], partner)

    def await_blocks(i, k):
        await_bytes(got[k].at[pl.ds(0, LAYERS), 0], g_recv.at[i, k])

    def new_rows(k, l, s, scale, take):
        start = pl.multiple_of((2 * chip_of(s) + core) * dims[k][0], dims[k][0])

        def run(i, carry):
            at = i * 16
            replicas[k][l, pl.ds(pl.multiple_of(start + at, 16), 16), :] = take(pl.ds(pl.multiple_of(at, 16), 16), scale).astype(jnp.bfloat16)
            return carry

        lax.fori_loop(0, dims[k][0] // 16, run, 0)

    for g, kinds in enumerate(NORM_GROUPS):
        roots = jnp.sqrt(shared(g))
        scales = {(k, l): LEARN_RATE * (pick(roots, 2 * k + l) / pick(roots, 8 + 2 * k + l)) for k in kinds for l in range(LAYERS)}
        if g == 0:
            await_bytes(early_w, early_sem.at[0])
        for k in kinds:
            for l in range(LAYERS):

                def fresh_rows(r, scale):
                    fresh = wv[k][l, r, :] - scale * acc[k][l, ME, r, :]
                    wv[k][l, r, :] = fresh
                    return fresh

                new_rows(k, l, ME, scales[k, l], fresh_rows)
                own_copy(l, 1 if g == 0 else 0, k).start()
        if g == 0:
            first_scales = scales
            for l in range(LAYERS):
                half_copy(l, ME, first_kind).start()

    for k in later_kinds:
        for l in range(LAYERS):
            own_copy(l, 1, k).start()
            half_copy(l, ME, k).start()

    await_bytes(early_w, early_sem.at[1])
    await_bytes(early_u, early_sem.at[3])
    for l in range(LAYERS):
        new_rows(first_kind, l, first_nb[l], first_scales[first_kind, l], lambda r, scale: early_w[l, r, :] - scale * early_u[l, r, :])
        half_copy(l, first_nb[l], first_kind).start()
    for k in later_kinds:
        await_blocks(0, k)
        for l in range(LAYERS):
            if k != later_kinds[0]:
                pass_copy(l, k).start()
            half_copy(l, first_nb[l], k).start()
    for l in range(LAYERS):
        pass_copy(l, later_kinds[0]).start()
    half = dims[first_kind][0] // 2

    def part_block(l, s, upper):
        start = pl.multiple_of((2 * chip_of(s) + core) * dims[first_kind][0] + upper * half, half)
        return replicas[first_kind].at[l, pl.ds(start, half)]

    def last_copy(l, other_core):
        src = part_block(l, first_nb[l], 1)
        send = h_send if other_core else g_send
        return remote(src, src, send.at[first_kind], tail_sem.at[other_core], device(second_nb[l], bool(other_core)))

    for l in range(LAYERS):
        src = part_block(l, first_nb[l], 0)
        remote(src, src, g_send.at[first_kind], g_recv.at[2, first_kind], second_dev[l]).start()
    for l in range(LAYERS):
        for other_core in range(2):
            last_copy(l, other_core).start()
    for k in KIND_ORDER:
        await_blocks(1, k)
        for l in range(LAYERS):
            half_copy(l, second_nb[l], k).start()
    for k in later_kinds[1:] + later_kinds[:1]:
        await_blocks(2, k)
        for l in range(LAYERS):
            half_copy(l, DG, k).start()
    half_bytes = got[first_kind].at[pl.ds(0, LAYERS), 0, pl.ds(0, half)]
    await_bytes(half_bytes, g_recv.at[2, first_kind])
    for l in range(LAYERS):
        src = part_block(l, DG, 0)
        remote(src, src, h_send.at[first_kind], h_recv.at[first_kind], partner).start()
    for other_core in range(2):
        await_bytes(half_bytes, tail_sem.at[other_core])

    for k in range(KINDS):
        if k == first_kind:
            await_bytes(sent[k].at[pl.ds(0, LAYERS), pl.ds(0, 3)], d_send.at[k])
            await_bytes(p1[k].at[pl.ds(0, LAYERS), 1], p1_send.at[k])
        else:
            await_bytes(sent[k], d_send.at[k])
            await_bytes(p1[k], p1_send.at[k])
        await_bytes(p2[k], p2_send.at[k])
        await_bytes(got[k].at[pl.ds(0, LAYERS), pl.ds(0, 2 if k == first_kind else 3)], g_send.at[k])
        await_bytes(got[k], h_send.at[k])
        if k == first_kind:
            await_bytes(replicas[2].at[0, pl.ds(0, LAYERS * 7 * half)], h_recv.at[k])
        else:
            await_bytes(got[k], h_recv.at[k])
    await_bytes(raw_in, raw_sem.at[0])
    await_bytes(raw_peer, raw_sem.at[2])
    await_bytes(early_u, early_sem.at[2])
    await_bytes(all_ref.at[pl.ds(0, GROUPS + 1), pl.ds(0, n_dev - 1)], ps_send.at[0])


def write_out(count, *refs):
    srcs, dsts, sems = refs[:count], refs[count:2 * count], refs[2 * count]
    pieces = 4
    for i, (src, dst) in enumerate(zip(srcs, dsts)):
        rows = src.shape[1] // pieces
        for l in range(LAYERS):
            for h in range(pieces):
                part = (l, pl.ds(h * rows, rows))
                pltpu.make_async_copy(src.at[part], dst.at[part], sems.at[i]).start()
    for i, (src, dst) in enumerate(zip(srcs, dsts)):
        pltpu.make_async_copy(src, dst, sems.at[i]).wait()


def solution(mesh):
    n_model, n_data = mesh.shape["model"], mesh.shape["data"]
    in_specs = []
    for col_split in COLUMN_SPLIT:
        in_specs.extend([grad_spec(col_split), state_spec(col_split), state_spec(col_split), state_spec(col_split)])
    out_specs = tuple([replica_spec(col_split) for col_split in COLUMN_SPLIT] + [state_spec(col_split) for col_split in COLUMN_SPLIT] * 3)

    def device_step(*arrays):
        dims = [arrays[4 * k + 1].shape[1:] for k in range(KINDS)]
        f32, bf16 = jnp.float32, jnp.bfloat16
        out_shape = [jax.ShapeDtypeStruct((LAYERS, n_data * d[0], d[1]), bf16) for d in dims]
        out_shape += [jax.ShapeDtypeStruct((LAYERS,) + tuple(d), f32) for d in dims] * 3

        def each(prefix, dtype):
            return [pltpu.VMEM(prefix + tuple(d), dtype) for d in dims]

        dma = pltpu.SemaphoreType.DMA
        n_dev = n_model * n_data
        scratch = (each((LAYERS, 4), f32) + each((LAYERS,), f32) + each((LAYERS, 4), bf16) + each((LAYERS, 4), bf16)
                   + each((LAYERS, 2), f32) + each((LAYERS,), f32))
        scratch += [pltpu.VMEM((GROUPS + 1, 1, 128), f32), pltpu.VMEM((GROUPS + 1, n_dev, 1, 128), f32)]
        scratch += [dma((4, 2)), dma((4,)), dma((4,)), dma((4, 4)), dma((4,)), dma((2, 4)), dma((4,)), dma((4,)),
                    dma((4,)), dma((3, 4)), dma((4,)), dma((4,)), dma((1,)), dma((GROUPS + 1,)), dma((4,)), dma((4,)), dma((2,)), pltpu.SemaphoreType.REGULAR((n_model + 1,))]
        first = tuple(dims[KIND_ORDER[0]])
        scratch += [pltpu.VMEM((LAYERS, 2) + first, bf16), pltpu.VMEM((LAYERS, 2) + first, bf16), pltpu.VMEM((LAYERS,) + first, bf16)]
        scratch += [pltpu.VMEM((LAYERS,) + first, f32)] * 2
        held = pl.pallas_call(
            functools.partial(kernel, n_model, n_data, dims),
            out_shape=[pltpu.VMEM(o.shape, o.dtype) for o in out_shape],
            in_specs=[pl.BlockSpec(memory_space=pl.ANY)] * 16,
            out_specs=[pl.BlockSpec(memory_space=pltpu.VMEM)] * 16,
            scratch_shapes=scratch,
            compiler_params=pltpu.CompilerParams(collective_id=0, has_side_effects=True, vmem_limit_bytes=COMM_VMEM),
            name="lamb_step",
        )(*arrays)
        held = [pltpu.with_memory_space_constraint(h, pltpu.VMEM) for h in held]
        return tuple(pl.pallas_call(
            functools.partial(write_out, len(out_shape)),
            out_shape=out_shape,
            in_specs=[pl.BlockSpec(memory_space=pltpu.VMEM)] * 16,
            out_specs=[pl.BlockSpec(memory_space=pl.ANY)] * 16,
            scratch_shapes=[dma((16,))],
            compiler_params=pltpu.CompilerParams(vmem_limit_bytes=1 << 20),
            name="write_out",
        )(*held))

    return jax.shard_map(device_step, mesh=mesh, in_specs=tuple(in_specs), out_specs=out_specs, check_vma=False)
```

```python
import functools

import jax
import jax.numpy as jnp
from jax import lax
from jax.experimental import pallas as pl
from jax.experimental.pallas import tpu as pltpu
from jax.sharding import PartitionSpec as P

LEARN_RATE = 0.08
BETA_ONE = 0.9
BETA_TWO = 0.999
ADAM_EPS = 1e-6
DECAY_RATE = 0.01
MAX_NORM = 1.0
STEP_COUNT = 100
TINY = 1e-36
COLUMN_SPLIT = (True, False, True, False)

KINDS = 4
LAYERS = 2
KIND_ORDER = (1, 0, 2, 3)
NORM_GROUPS = ((1,), (0,), (2, 3))
GROUPS = len(NORM_GROUPS)
ME, XN, YN, DG = 0, 1, 2, 3
MESH = pl.DeviceIdType.MESH
COMM_VMEM = 42 << 20


def grad_spec(col_split):
    return P("data", None, None, "model") if col_split else P("data", None, "model", None)


def state_spec(col_split):
    return P(None, "data", "model") if col_split else P(None, ("model", "data"), None)


def replica_spec(col_split):
    return P(None, None, "model") if col_split else P(None, "model", None)


def lane_fold(x):
    total = x[:, 0:128]
    for j in range(1, x.shape[1] // 128):
        total = total + x[:, 128 * j:128 * (j + 1)]
    return total


def kernel(n_model, n_data, dims, *refs):
    n_dev = n_model * n_data
    grads, weights, firsts, seconds = ([refs[4 * k + i] for k in range(KINDS)] for i in range(4))
    outs = refs[16:32]
    replicas, wv, mv, vv = outs[0:4], outs[4:8], outs[8:12], outs[12:16]
    scratch = refs[32:]
    acc, stage, sent, got, p1, p2 = (scratch[4 * i:4 * i + 4] for i in range(6))
    (row_ref, all_ref, ld_unit, ld_state, d_send, d_recv, p1_send, p1_recv, p2_send, p2_recv,
     g_send, g_recv, h_send, h_recv, ps_send, ps_recv, raw_sem, early_sem, tail_sem, rounds,
     raw_out, raw_in, raw_peer, early_w, early_u) = scratch[24:]

    model = lax.axis_index("model")
    data = lax.axis_index("data")
    core = data % 2
    xc = (data // 2) % 2
    yc = data // 4
    me = model * n_data + data

    def chip_of(slot):
        x = xc if slot in (ME, YN) else 1 - xc
        y = yc if slot in (ME, XN) else 1 - yc
        return 2 * y + x

    def device(slot, other_core=False):
        return (model, 2 * chip_of(slot) + ((1 - core) if other_core else core))

    partner = device(ME, True)
    to_x = device(XN)
    to_y = device(YN)

    def rows_of(k, slot, other_core):
        rows = dims[k][0]
        return pl.ds(pl.multiple_of((2 * chip_of(slot) + ((1 - core) if other_core else core)) * rows, rows), rows)

    def load_unit(l, s, k):
        pltpu.make_async_copy(grads[k].at[0, l, rows_of(k, s, True)], stage[k].at[l], ld_unit.at[k, l]).start()
        pltpu.make_async_copy(grads[k].at[0, l, rows_of(k, s, False)], acc[k].at[l, s], ld_unit.at[k, l]).start()

    def remote(src, dst, send, recv, dev):
        return pltpu.make_async_remote_copy(src_ref=src, dst_ref=dst, send_sem=send, recv_sem=recv, device_id=dev, device_id_type=MESH)

    def await_bytes(ref, sem):
        pltpu.make_async_copy(ref, ref, sem).wait()

    first_dev = (to_x, to_y)
    second_dev = (to_y, to_x)
    first_nb = (XN, YN)
    second_nb = (YN, XN)

    def over_rows(k, step, body):
        def run(i, carry):
            body(pl.ds(pl.multiple_of(i * step, step), step))
            return carry

        lax.fori_loop(0, dims[k][0] // step, run, 0)

    def sum_rows(k, body):
        rows, cols = dims[k]

        def run(i, carry):
            r = pl.ds(pl.multiple_of(i * 8, 8), 8)
            return tuple(carry[l] + body(l, r) for l in range(LAYERS))

        sums = lax.fori_loop(0, rows // 8, run, (jnp.zeros((8, cols), jnp.float32),) * LAYERS)
        return [lane_fold(x) for x in sums]

    pairs = [(slots, k) for slots in ((DG, DG), (YN, XN), (XN, YN), (ME, ME)) for k in KIND_ORDER]
    ahead = 3

    def load_pair(slots, k):
        for l in range(LAYERS):
            load_unit(l, slots[l], k)

    barrier = pltpu.get_barrier_semaphore()
    z_hops = jnp.minimum(model, 1) + jnp.minimum(n_model - 1 - model, 1)

    def greet_z(sem):
        @pl.when(model > 0)
        def _():
            pl.semaphore_signal(sem, inc=1, device_id=(model - 1, data), device_id_type=MESH)

        @pl.when(model < n_model - 1)
        def _():
            pl.semaphore_signal(sem, inc=1, device_id=(model + 1, data), device_id_type=MESH)

    for dev in (partner, to_x, to_y):
        pl.semaphore_signal(barrier, inc=1, device_id=dev, device_id_type=MESH)
    greet_z(barrier)
    for p in pairs[:ahead]:
        load_pair(*p)

    first_kind = KIND_ORDER[0]
    later_kinds = KIND_ORDER[1:]

    def cast_rows(k, l, s):
        def body(r):
            sent[k][l, s, r, :] = stage[k][l, r, :].astype(jnp.bfloat16)

        over_rows(k, 16, body)

    def await_unit(k, l):
        await_bytes(acc[k].at[l, pl.ds(0, 2)], ld_unit.at[k, l])

    for l in range(LAYERS):
        await_unit(first_kind, l)

        def body(r):
            raw_out[l, 0, r, :] = acc[first_kind][l, DG, r, :].astype(jnp.bfloat16)
            raw_out[l, 1, r, :] = stage[first_kind][l, r, :].astype(jnp.bfloat16)

        over_rows(first_kind, 16, body)
    load_pair(*pairs[ahead])
    for l in range(LAYERS):
        await_unit(pairs[1][1], l)
        cast_rows(pairs[1][1], l, pairs[1][0][l])

    pl.semaphore_wait(barrier, 3 + z_hops)
    for l in range(LAYERS):
        remote(raw_out.at[l], raw_in.at[l], raw_sem.at[0], raw_sem.at[1], first_dev[l]).start()

    def pair_send(g, slots, k):
        for l in range(LAYERS):
            remote(sent[k].at[l, slots[l]], got[k].at[l, slots[l]], d_send.at[k], d_recv.at[g, k], partner).start()

    pair_send(0, *pairs[1])
    axes = ("z",) * (n_model - 2) + ("core", "x", "y")
    n_rounds = len(axes)

    def greet_round(r):
        if axes[r] == "z":
            greet_z(rounds.at[r])
        else:
            pl.semaphore_signal(rounds.at[r], inc=1, device_id={"core": partner, "x": to_x, "y": to_y}[axes[r]], device_id_type=MESH)

    greet_round(0)

    def next_round(r):
        pl.semaphore_wait(rounds.at[r], z_hops if axes[r] == "z" else 1)
        if r + 1 < n_rounds:
            greet_round(r + 1)

    def load_state(k):
        for src, dst in ((weights, wv), (firsts, mv), (seconds, vv)):
            pltpu.make_async_copy(src[k], dst[k], ld_state.at[k]).start()

    def pair_half(g, slots, k):
        for l in range(LAYERS):
            await_unit(k, l)
            cast_rows(k, l, slots[l])
        pair_send(g, slots, k)

    def chip_half(g, slots, k):
        await_bytes(got[k].at[pl.ds(0, LAYERS), 0], d_recv.at[g, k])
        for l in range(LAYERS):
            s = slots[l]

            def body(r):
                own = acc[k][l, s, r, :].astype(jnp.bfloat16).astype(jnp.float32)
                acc[k][l, s, r, :] = own + got[k][l, s, r, :].astype(jnp.float32)

            over_rows(k, 16, body)
            if s == DG or s == first_nb[l]:
                t = 0 if s == DG else 1
                remote(acc[k].at[l, s], p1[k].at[l, t], p1_send.at[k], p1_recv.at[t, k], first_dev[l]).start()

    for i in range(1, len(pairs) + 1):
        if i < len(pairs):
            if i >= 2:
                pair_half(i // KINDS, *pairs[i])
            if i + ahead < len(pairs):
                load_pair(*pairs[i + ahead])
            else:
                for k in (KIND_ORDER[i + ahead - len(pairs)],) + ((KIND_ORDER[ahead],) if i + 1 == len(pairs) else ()):
                    load_state(k)
        if i >= 2:
            chip_half((i - 1) // KINDS, *pairs[i - 1])
        if i >= 4 and i % 2 == 0 and (i - 4) // 2 < n_rounds:
            next_round((i - 4) // 2)

    await_bytes(raw_in, raw_sem.at[1])
    for l in range(LAYERS):
        remote(raw_in.at[l, 1], raw_peer.at[l], raw_sem.at[2], raw_sem.at[3], partner).start()
    for k in later_kinds + (first_kind,):
        if k == first_kind:
            await_bytes(raw_peer, raw_sem.at[3])
        else:
            await_bytes(p1[k].at[pl.ds(0, LAYERS), 0], p1_recv.at[0, k])
        for l in range(LAYERS):
            s = second_nb[l]

            def body(r):
                if k == first_kind:
                    come = raw_in[l, 0, r, :].astype(jnp.float32) + raw_peer[l, r, :].astype(jnp.float32)
                else:
                    come = p1[k][l, 0, r, :]
                acc[k][l, s, r, :] = acc[k][l, s, r, :] + come

            over_rows(k, 16, body)
            remote(acc[k].at[l, s], p2[k].at[l], p2_send.at[k], p2_recv.at[k], second_dev[l]).start()

    def share(which, row):
        row_ref[which] = row
        all_ref[which, me] = row
        for dz in sorted(range(n_model), key=lambda z: -min(z, n_model - z)):
            for dd in reversed(range(n_data)):
                if dz or dd:
                    remote(row_ref.at[which], all_ref.at[which, me], ps_send.at[0], ps_recv.at[which],
                           ((model + dz) % n_model, (data + dd) % n_data)).start()

    def shared(which):
        await_bytes(all_ref.at[which, pl.ds(0, n_dev - 1)], ps_recv.at[which])
        parts = [jnp.sum(all_ref[which, pl.ds(i, n_dev // 4)], axis=0) for i in range(0, n_dev, n_dev // 4)]
        return (parts[0] + parts[1]) + (parts[2] + parts[3])

    lane = lax.broadcasted_iota(jnp.int32, (1, 128), 1)

    def put(i, part):
        return jnp.where(lane == i, jnp.sum(part, keepdims=True), 0.0)

    def pick(row, i):
        return jnp.sum(jnp.where(lane == i, row, 0.0), axis=1, keepdims=True)

    norms = jnp.zeros((1, 128), jnp.float32)
    for k in KIND_ORDER:
        await_bytes(acc[k].at[pl.ds(0, LAYERS), pl.ds(0, 3)], ld_state.at[k])
        for l, part in enumerate(sum_rows(k, lambda l, r: wv[k][l, r, :] * wv[k][l, r, :])):
            norms = norms + put(2 * k + l, part)

    for k in KIND_ORDER:
        await_bytes(p1[k].at[pl.ds(0, LAYERS), 0], p1_recv.at[1, k])
        for l in range(LAYERS):

            def body(r):
                acc[k][l, ME, r, :] = acc[k][l, ME, r, :] + p1[k][l, 1, r, :]

            over_rows(k, 8, body)

    grad_sq = jnp.zeros((8, 128), jnp.float32)
    for k in later_kinds + (first_kind,):
        await_bytes(p2[k], p2_recv.at[k])

        def body(l, r):
            mean = (acc[k][l, ME, r, :] + p2[k][l, r, :]) * (1.0 / n_data)
            acc[k][l, ME, r, :] = mean
            return mean * mean

        for part in sum_rows(k, body):
            grad_sq = grad_sq + part
    share(GROUPS, jnp.sum(grad_sq, axis=0, keepdims=True))

    for l in range(LAYERS):
        remote(wv[first_kind].at[l], early_w.at[l], early_sem.at[0], early_sem.at[1], first_dev[l]).start()
    total_sq = jnp.sum(shared(GROUPS), axis=1, keepdims=True)
    clip = jnp.minimum(1.0, MAX_NORM / jnp.sqrt(total_sq))
    first_gain = (1.0 - BETA_ONE) * clip
    second_gain = (1.0 - BETA_TWO) * clip * clip
    root_scale = (1.0 - BETA_TWO ** STEP_COUNT) ** 0.5
    hat_scale = root_scale / (1.0 - BETA_ONE ** STEP_COUNT)

    def updates(k):
        def body(l, r):
            mean = acc[k][l, ME, r, :]
            first = BETA_ONE * mv[k][l, r, :] + first_gain * mean
            second = BETA_TWO * vv[k][l, r, :] + second_gain * (mean * mean)
            mv[k][l, r, :] = first
            vv[k][l, r, :] = second
            shifted = second + TINY
            root = shifted * lax.rsqrt(shifted)
            update = (hat_scale * first) / (root + ADAM_EPS * root_scale) + DECAY_RATE * wv[k][l, r, :]
            acc[k][l, ME, r, :] = update
            return update * update

        return sum_rows(k, body)

    for g, kinds in enumerate(NORM_GROUPS):
        squares = norms
        for k in kinds:
            for l, part in enumerate(updates(k)):
                squares = squares + put(8 + 2 * k + l, part)
        share(g, squares)
        if g < 2:
            half = dims[first_kind][0] // 2
            piece = pl.ds(g * half, half)
            for l in range(LAYERS):
                remote(acc[first_kind].at[l, ME, piece], early_u.at[l, piece], early_sem.at[2], early_sem.at[3], first_dev[l]).start()

    def block(l, s, k):
        return replicas[k].at[l, rows_of(k, s, False)]

    def own_copy(l, second, k):
        return remote(block(l, ME, k), block(l, ME, k), g_send.at[k], g_recv.at[second, k], second_dev[l] if second else first_dev[l])

    def pass_copy(l, k):
        src = block(l, first_nb[l], k)
        return remote(src, src, g_send.at[k], g_recv.at[2, k], second_dev[l])

    def half_copy(l, s, k):
        return remote(block(l, s, k), block(l, s, k), h_send.at[k], h_recv.at[k], partner)

    def await_blocks(i, k):
        await_bytes(got[k].at[pl.ds(0, LAYERS), 0], g_recv.at[i, k])

    def new_rows(k, l, s, scale, take):
        start = pl.multiple_of((2 * chip_of(s) + core) * dims[k][0], dims[k][0])

        def run(i, carry):
            at = i * 16
            replicas[k][l, pl.ds(pl.multiple_of(start + at, 16), 16), :] = take(pl.ds(pl.multiple_of(at, 16), 16), scale).astype(jnp.bfloat16)
            return carry

        lax.fori_loop(0, dims[k][0] // 16, run, 0)

    for g, kinds in enumerate(NORM_GROUPS):
        roots = jnp.sqrt(shared(g))
        scales = {(k, l): LEARN_RATE * (pick(roots, 2 * k + l) / pick(roots, 8 + 2 * k + l)) for k in kinds for l in range(LAYERS)}
        if g == 0:
            await_bytes(early_w, early_sem.at[0])
        for k in kinds:
            for l in range(LAYERS):

                def fresh_rows(r, scale):
                    fresh = wv[k][l, r, :] - scale * acc[k][l, ME, r, :]
                    wv[k][l, r, :] = fresh
                    return fresh

                new_rows(k, l, ME, scales[k, l], fresh_rows)
                own_copy(l, 1 if g == 0 else 0, k).start()
        if g == 0:
            first_scales = scales
            for l in range(LAYERS):
                half_copy(l, ME, first_kind).start()

    for k in later_kinds:
        for l in range(LAYERS):
            own_copy(l, 1, k).start()
            half_copy(l, ME, k).start()

    await_bytes(early_w, early_sem.at[1])
    await_bytes(early_u, early_sem.at[3])
    for l in range(LAYERS):
        new_rows(first_kind, l, first_nb[l], first_scales[first_kind, l], lambda r, scale: early_w[l, r, :] - scale * early_u[l, r, :])
        half_copy(l, first_nb[l], first_kind).start()
    for k in later_kinds:
        await_blocks(0, k)
        for l in range(LAYERS):
            if k != later_kinds[0]:
                pass_copy(l, k).start()
            half_copy(l, first_nb[l], k).start()
    for l in range(LAYERS):
        pass_copy(l, later_kinds[0]).start()
    half = dims[first_kind][0] // 2

    def part_block(l, s, upper):
        start = pl.multiple_of((2 * chip_of(s) + core) * dims[first_kind][0] + upper * half, half)
        return replicas[first_kind].at[l, pl.ds(start, half)]

    def last_copy(l, other_core):
        src = part_block(l, first_nb[l], 1)
        send = h_send if other_core else g_send
        return remote(src, src, send.at[first_kind], tail_sem.at[other_core], device(second_nb[l], bool(other_core)))

    for l in range(LAYERS):
        src = part_block(l, first_nb[l], 0)
        remote(src, src, g_send.at[first_kind], g_recv.at[2, first_kind], second_dev[l]).start()
    for l in range(LAYERS):
        for other_core in range(2):
            last_copy(l, other_core).start()
    for k in KIND_ORDER:
        await_blocks(1, k)
        for l in range(LAYERS):
            half_copy(l, second_nb[l], k).start()
    for k in later_kinds[1:] + later_kinds[:1]:
        await_blocks(2, k)
        for l in range(LAYERS):
            half_copy(l, DG, k).start()
    half_bytes = got[first_kind].at[pl.ds(0, LAYERS), 0, pl.ds(0, half)]
    await_bytes(half_bytes, g_recv.at[2, first_kind])
    for l in range(LAYERS):
        src = part_block(l, DG, 0)
        remote(src, src, h_send.at[first_kind], h_recv.at[first_kind], partner).start()
    for other_core in range(2):
        await_bytes(half_bytes, tail_sem.at[other_core])

    for k in range(KINDS):
        if k == first_kind:
            await_bytes(sent[k].at[pl.ds(0, LAYERS), pl.ds(0, 3)], d_send.at[k])
            await_bytes(p1[k].at[pl.ds(0, LAYERS), 1], p1_send.at[k])
        else:
            await_bytes(sent[k], d_send.at[k])
            await_bytes(p1[k], p1_send.at[k])
        await_bytes(p2[k], p2_send.at[k])
        await_bytes(got[k].at[pl.ds(0, LAYERS), pl.ds(0, 2 if k == first_kind else 3)], g_send.at[k])
        await_bytes(got[k], h_send.at[k])
        if k == first_kind:
            await_bytes(replicas[2].at[0, pl.ds(0, LAYERS * 7 * half)], h_recv.at[k])
        else:
            await_bytes(got[k], h_recv.at[k])
    await_bytes(raw_in, raw_sem.at[0])
    await_bytes(raw_peer, raw_sem.at[2])
    await_bytes(early_u, early_sem.at[2])
    await_bytes(all_ref.at[pl.ds(0, GROUPS + 1), pl.ds(0, n_dev - 1)], ps_send.at[0])


def write_out(count, *refs):
    srcs, dsts, sems = refs[:count], refs[count:2 * count], refs[2 * count]
    pieces = 4
    for i, (src, dst) in enumerate(zip(srcs, dsts)):
        rows = src.shape[1] // pieces
        for l in range(LAYERS):
            for h in range(pieces):
                part = (l, pl.ds(h * rows, rows))
                pltpu.make_async_copy(src.at[part], dst.at[part], sems.at[i]).start()
    for i, (src, dst) in enumerate(zip(srcs, dsts)):
        pltpu.make_async_copy(src, dst, sems.at[i]).wait()


def solution(mesh):
    n_model, n_data = mesh.shape["model"], mesh.shape["data"]
    in_specs = []
    for col_split in COLUMN_SPLIT:
        in_specs.extend([grad_spec(col_split), state_spec(col_split), state_spec(col_split), state_spec(col_split)])
    out_specs = tuple([replica_spec(col_split) for col_split in COLUMN_SPLIT] + [state_spec(col_split) for col_split in COLUMN_SPLIT] * 3)

    def device_step(*arrays):
        dims = [arrays[4 * k + 1].shape[1:] for k in range(KINDS)]
        f32, bf16 = jnp.float32, jnp.bfloat16
        out_shape = [jax.ShapeDtypeStruct((LAYERS, n_data * d[0], d[1]), bf16) for d in dims]
        out_shape += [jax.ShapeDtypeStruct((LAYERS,) + tuple(d), f32) for d in dims] * 3

        def each(prefix, dtype):
            return [pltpu.VMEM(prefix + tuple(d), dtype) for d in dims]

        dma = pltpu.SemaphoreType.DMA
        n_dev = n_model * n_data
        scratch = (each((LAYERS, 4), f32) + each((LAYERS,), f32) + each((LAYERS, 4), bf16) + each((LAYERS, 4), bf16)
                   + each((LAYERS, 2), f32) + each((LAYERS,), f32))
        scratch += [pltpu.VMEM((GROUPS + 1, 1, 128), f32), pltpu.VMEM((GROUPS + 1, n_dev, 1, 128), f32)]
        scratch += [dma((4, 2)), dma((4,)), dma((4,)), dma((4, 4)), dma((4,)), dma((2, 4)), dma((4,)), dma((4,)),
                    dma((4,)), dma((3, 4)), dma((4,)), dma((4,)), dma((1,)), dma((GROUPS + 1,)), dma((4,)), dma((4,)), dma((2,)), pltpu.SemaphoreType.REGULAR((n_model + 1,))]
        first = tuple(dims[KIND_ORDER[0]])
        scratch += [pltpu.VMEM((LAYERS, 2) + first, bf16), pltpu.VMEM((LAYERS, 2) + first, bf16), pltpu.VMEM((LAYERS,) + first, bf16)]
        scratch += [pltpu.VMEM((LAYERS,) + first, f32)] * 2
        held = pl.pallas_call(
            functools.partial(kernel, n_model, n_data, dims),
            out_shape=[pltpu.VMEM(o.shape, o.dtype) for o in out_shape],
            in_specs=[pl.BlockSpec(memory_space=pl.ANY)] * 16,
            out_specs=[pl.BlockSpec(memory_space=pltpu.VMEM)] * 16,
            scratch_shapes=scratch,
            compiler_params=pltpu.CompilerParams(collective_id=0, has_side_effects=True, vmem_limit_bytes=COMM_VMEM),
            name="lamb_step",
        )(*arrays)
        held = [pltpu.with_memory_space_constraint(h, pltpu.VMEM) for h in held]
        return tuple(pl.pallas_call(
            functools.partial(write_out, len(out_shape)),
            out_shape=out_shape,
            in_specs=[pl.BlockSpec(memory_space=pltpu.VMEM)] * 16,
            out_specs=[pl.BlockSpec(memory_space=pl.ANY)] * 16,
            scratch_shapes=[dma((16,))],
            compiler_params=pltpu.CompilerParams(vmem_limit_bytes=1 << 20),
            name="write_out",
        )(*held))

    return jax.shard_map(device_step, mesh=mesh, in_specs=tuple(in_specs), out_specs=out_specs, check_vma=False)
```

```python
import functools

import jax
import jax.numpy as jnp
from jax import lax
from jax.experimental import pallas as pl
from jax.experimental.pallas import tpu as pltpu
from jax.sharding import PartitionSpec as P

LEARN_RATE = 0.08
BETA_ONE = 0.9
BETA_TWO = 0.999
ADAM_EPS = 1e-6
DECAY_RATE = 0.01
MAX_NORM = 1.0
STEP_COUNT = 100
TINY = 1e-36
COLUMN_SPLIT = (True, False, True, False)

KINDS = 4
LAYERS = 2
KIND_ORDER = (1, 0, 2, 3)
NORM_GROUPS = ((1,), (0,), (2, 3))
GROUPS = len(NORM_GROUPS)
ME, XN, YN, DG = 0, 1, 2, 3
MESH = pl.DeviceIdType.MESH
COMM_VMEM = 42 << 20


def grad_spec(col_split):
    return P("data", None, None, "model") if col_split else P("data", None, "model", None)


def state_spec(col_split):
    return P(None, "data", "model") if col_split else P(None, ("model", "data"), None)


def replica_spec(col_split):
    return P(None, None, "model") if col_split else P(None, "model", None)


def lane_fold(x):
    total = x[:, 0:128]
    for j in range(1, x.shape[1] // 128):
        total = total + x[:, 128 * j:128 * (j + 1)]
    return total


def kernel(n_model, n_data, dims, *refs):
    n_dev = n_model * n_data
    grads, weights, firsts, seconds = ([refs[4 * k + i] for k in range(KINDS)] for i in range(4))
    outs = refs[16:32]
    replicas, wv, mv, vv = outs[0:4], outs[4:8], outs[8:12], outs[12:16]
    scratch = refs[32:]
    acc, stage, sent, got, p1, p2 = (scratch[4 * i:4 * i + 4] for i in range(6))
    (row_ref, all_ref, ld_unit, ld_state, d_send, d_recv, p1_send, p1_recv, p2_send, p2_recv,
     g_send, g_recv, h_send, h_recv, ps_send, ps_recv, raw_sem, early_sem, tail_sem, rounds,
     raw_out, raw_in, raw_peer, early_w, early_u) = scratch[24:]

    model = lax.axis_index("model")
    data = lax.axis_index("data")
    core = data % 2
    xc = (data // 2) % 2
    yc = data // 4
    me = model * n_data + data

    def chip_of(slot):
        x = xc if slot in (ME, YN) else 1 - xc
        y = yc if slot in (ME, XN) else 1 - yc
        return 2 * y + x

    def device(slot, other_core=False):
        return (model, 2 * chip_of(slot) + ((1 - core) if other_core else core))

    partner = device(ME, True)
    to_x = device(XN)
    to_y = device(YN)

    def rows_of(k, slot, other_core):
        rows = dims[k][0]
        return pl.ds(pl.multiple_of((2 * chip_of(slot) + ((1 - core) if other_core else core)) * rows, rows), rows)

    def load_unit(l, s, k):
        pltpu.make_async_copy(grads[k].at[0, l, rows_of(k, s, True)], stage[k].at[l], ld_unit.at[k, l]).start()
        pltpu.make_async_copy(grads[k].at[0, l, rows_of(k, s, False)], acc[k].at[l, s], ld_unit.at[k, l]).start()

    def remote(src, dst, send, recv, dev):
        return pltpu.make_async_remote_copy(src_ref=src, dst_ref=dst, send_sem=send, recv_sem=recv, device_id=dev, device_id_type=MESH)

    def await_bytes(ref, sem):
        pltpu.make_async_copy(ref, ref, sem).wait()

    first_dev = (to_x, to_y)
    second_dev = (to_y, to_x)
    first_nb = (XN, YN)
    second_nb = (YN, XN)

    def over_rows(k, step, body):
        def run(i, carry):
            body(pl.ds(pl.multiple_of(i * step, step), step))
            return carry

        lax.fori_loop(0, dims[k][0] // step, run, 0)

    def sum_rows(k, body):
        rows, cols = dims[k]

        def run(i, carry):
            r = pl.ds(pl.multiple_of(i * 8, 8), 8)
            return tuple(carry[l] + body(l, r) for l in range(LAYERS))

        sums = lax.fori_loop(0, rows // 8, run, (jnp.zeros((8, cols), jnp.float32),) * LAYERS)
        return [lane_fold(x) for x in sums]

    pairs = [(slots, k) for slots in ((DG, DG), (YN, XN), (XN, YN), (ME, ME)) for k in KIND_ORDER]
    ahead = 3

    def load_pair(slots, k):
        for l in range(LAYERS):
            load_unit(l, slots[l], k)

    barrier = pltpu.get_barrier_semaphore()
    z_hops = jnp.minimum(model, 1) + jnp.minimum(n_model - 1 - model, 1)

    def greet_z(sem):
        @pl.when(model > 0)
        def _():
            pl.semaphore_signal(sem, inc=1, device_id=(model - 1, data), device_id_type=MESH)

        @pl.when(model < n_model - 1)
        def _():
            pl.semaphore_signal(sem, inc=1, device_id=(model + 1, data), device_id_type=MESH)

    for dev in (partner, to_x, to_y):
        pl.semaphore_signal(barrier, inc=1, device_id=dev, device_id_type=MESH)
    greet_z(barrier)
    for p in pairs[:ahead]:
        load_pair(*p)

    first_kind = KIND_ORDER[0]
    later_kinds = KIND_ORDER[1:]

    def cast_rows(k, l, s):
        def body(r):
            sent[k][l, s, r, :] = stage[k][l, r, :].astype(jnp.bfloat16)

        over_rows(k, 16, body)

    def await_unit(k, l):
        await_bytes(acc[k].at[l, pl.ds(0, 2)], ld_unit.at[k, l])

    for l in range(LAYERS):
        await_unit(first_kind, l)

        def body(r):
            raw_out[l, 0, r, :] = acc[first_kind][l, DG, r, :].astype(jnp.bfloat16)
            raw_out[l, 1, r, :] = stage[first_kind][l, r, :].astype(jnp.bfloat16)

        over_rows(first_kind, 16, body)
    load_pair(*pairs[ahead])
    for l in range(LAYERS):
        await_unit(pairs[1][1], l)
        cast_rows(pairs[1][1], l, pairs[1][0][l])

    pl.semaphore_wait(barrier, 3 + z_hops)
    for l in range(LAYERS):
        remote(raw_out.at[l], raw_in.at[l], raw_sem.at[0], raw_sem.at[1], first_dev[l]).start()

    def pair_send(g, slots, k):
        for l in range(LAYERS):
            remote(sent[k].at[l, slots[l]], got[k].at[l, slots[l]], d_send.at[k], d_recv.at[g, k], partner).start()

    pair_send(0, *pairs[1])
    axes = ("z",) * (n_model - 2) + ("core", "x", "y")
    n_rounds = len(axes)

    def greet_round(r):
        if axes[r] == "z":
            greet_z(rounds.at[r])
        else:
            pl.semaphore_signal(rounds.at[r], inc=1, device_id={"core": partner, "x": to_x, "y": to_y}[axes[r]], device_id_type=MESH)

    greet_round(0)

    def next_round(r):
        pl.semaphore_wait(rounds.at[r], z_hops if axes[r] == "z" else 1)
        if r + 1 < n_rounds:
            greet_round(r + 1)

    def load_state(k):
        for src, dst in ((weights, wv), (firsts, mv), (seconds, vv)):
            pltpu.make_async_copy(src[k], dst[k], ld_state.at[k]).start()

    def pair_half(g, slots, k):
        for l in range(LAYERS):
            await_unit(k, l)
            cast_rows(k, l, slots[l])
        pair_send(g, slots, k)

    def chip_half(g, slots, k):
        await_bytes(got[k].at[pl.ds(0, LAYERS), 0], d_recv.at[g, k])
        for l in range(LAYERS):
            s = slots[l]

            def body(r):
                own = acc[k][l, s, r, :].astype(jnp.bfloat16).astype(jnp.float32)
                acc[k][l, s, r, :] = own + got[k][l, s, r, :].astype(jnp.float32)

            over_rows(k, 16, body)
            if s == DG or s == first_nb[l]:
                t = 0 if s == DG else 1
                remote(acc[k].at[l, s], p1[k].at[l, t], p1_send.at[k], p1_recv.at[t, k], first_dev[l]).start()

    for i in range(1, len(pairs) + 1):
        if i < len(pairs):
            if i >= 2:
                pair_half(i // KINDS, *pairs[i])
            if i + ahead < len(pairs):
                load_pair(*pairs[i + ahead])
            else:
                for k in (KIND_ORDER[i + ahead - len(pairs)],) + ((KIND_ORDER[ahead],) if i + 1 == len(pairs) else ()):
                    load_state(k)
        if i >= 2:
            chip_half((i - 1) // KINDS, *pairs[i - 1])
        if i >= 4 and i % 2 == 0 and (i - 4) // 2 < n_rounds:
            next_round((i - 4) // 2)

    await_bytes(raw_in, raw_sem.at[1])
    for l in range(LAYERS):
        remote(raw_in.at[l, 1], raw_peer.at[l], raw_sem.at[2], raw_sem.at[3], partner).start()
    for k in later_kinds + (first_kind,):
        if k == first_kind:
            await_bytes(raw_peer, raw_sem.at[3])
        else:
            await_bytes(p1[k].at[pl.ds(0, LAYERS), 0], p1_recv.at[0, k])
        for l in range(LAYERS):
            s = second_nb[l]

            def body(r):
                if k == first_kind:
                    come = raw_in[l, 0, r, :].astype(jnp.float32) + raw_peer[l, r, :].astype(jnp.float32)
                else:
                    come = p1[k][l, 0, r, :]
                acc[k][l, s, r, :] = acc[k][l, s, r, :] + come

            over_rows(k, 16, body)
            remote(acc[k].at[l, s], p2[k].at[l], p2_send.at[k], p2_recv.at[k], second_dev[l]).start()

    def share(which, row):
        row_ref[which] = row
        all_ref[which, me] = row
        for dz in sorted(range(n_model), key=lambda z: -min(z, n_model - z)):
            for dd in (3, 0, 2, 7, 4, 1, 5, 6):
                if dz or dd:
                    remote(row_ref.at[which], all_ref.at[which, me], ps_send.at[0], ps_recv.at[which],
                           ((model + dz) % n_model, (data + dd) % n_data)).start()

    def shared(which):
        await_bytes(all_ref.at[which, pl.ds(0, n_dev - 1)], ps_recv.at[which])
        parts = [jnp.sum(all_ref[which, pl.ds(i, n_dev // 4)], axis=0) for i in range(0, n_dev, n_dev // 4)]
        return (parts[0] + parts[1]) + (parts[2] + parts[3])

    lane = lax.broadcasted_iota(jnp.int32, (1, 128), 1)

    def put(i, part):
        return jnp.where(lane == i, jnp.sum(part, keepdims=True), 0.0)

    def pick(row, i):
        return jnp.sum(jnp.where(lane == i, row, 0.0), axis=1, keepdims=True)

    norms = jnp.zeros((1, 128), jnp.float32)
    for k in KIND_ORDER:
        await_bytes(acc[k].at[pl.ds(0, LAYERS), pl.ds(0, 3)], ld_state.at[k])
        for l, part in enumerate(sum_rows(k, lambda l, r: wv[k][l, r, :] * wv[k][l, r, :])):
            norms = norms + put(2 * k + l, part)

    for k in KIND_ORDER:
        await_bytes(p1[k].at[pl.ds(0, LAYERS), 0], p1_recv.at[1, k])
        for l in range(LAYERS):

            def body(r):
                acc[k][l, ME, r, :] = acc[k][l, ME, r, :] + p1[k][l, 1, r, :]

            over_rows(k, 8, body)

    grad_sq = jnp.zeros((8, 128), jnp.float32)
    for k in later_kinds + (first_kind,):
        await_bytes(p2[k], p2_recv.at[k])

        def body(l, r):
            mean = (acc[k][l, ME, r, :] + p2[k][l, r, :]) * (1.0 / n_data)
            acc[k][l, ME, r, :] = mean
            return mean * mean

        for part in sum_rows(k, body):
            grad_sq = grad_sq + part
    share(GROUPS, jnp.sum(grad_sq, axis=0, keepdims=True))

    for l in range(LAYERS):
        remote(wv[first_kind].at[l], early_w.at[l], early_sem.at[0], early_sem.at[1], first_dev[l]).start()
    total_sq = jnp.sum(shared(GROUPS), axis=1, keepdims=True)
    clip = jnp.minimum(1.0, MAX_NORM / jnp.sqrt(total_sq))
    first_gain = (1.0 - BETA_ONE) * clip
    second_gain = (1.0 - BETA_TWO) * clip * clip
    root_scale = (1.0 - BETA_TWO ** STEP_COUNT) ** 0.5
    hat_scale = root_scale / (1.0 - BETA_ONE ** STEP_COUNT)

    def updates(k):
        def body(l, r):
            mean = acc[k][l, ME, r, :]
            first = BETA_ONE * mv[k][l, r, :] + first_gain * mean
            second = BETA_TWO * vv[k][l, r, :] + second_gain * (mean * mean)
            mv[k][l, r, :] = first
            vv[k][l, r, :] = second
            shifted = second + TINY
            root = shifted * lax.rsqrt(shifted)
            update = (hat_scale * first) / (root + ADAM_EPS * root_scale) + DECAY_RATE * wv[k][l, r, :]
            acc[k][l, ME, r, :] = update
            return update * update

        return sum_rows(k, body)

    for g, kinds in enumerate(NORM_GROUPS):
        squares = norms
        for k in kinds:
            for l, part in enumerate(updates(k)):
                squares = squares + put(8 + 2 * k + l, part)
        share(g, squares)
        if g < 2:
            half = dims[first_kind][0] // 2
            piece = pl.ds(g * half, half)
            for l in range(LAYERS):
                remote(acc[first_kind].at[l, ME, piece], early_u.at[l, piece], early_sem.at[2], early_sem.at[3], first_dev[l]).start()

    def block(l, s, k):
        return replicas[k].at[l, rows_of(k, s, False)]

    def own_copy(l, second, k):
        return remote(block(l, ME, k), block(l, ME, k), g_send.at[k], g_recv.at[second, k], second_dev[l] if second else first_dev[l])

    def pass_copy(l, k):
        src = block(l, first_nb[l], k)
        return remote(src, src, g_send.at[k], g_recv.at[2, k], second_dev[l])

    def half_copy(l, s, k):
        return remote(block(l, s, k), block(l, s, k), h_send.at[k], h_recv.at[k], partner)

    def await_blocks(i, k):
        await_bytes(got[k].at[pl.ds(0, LAYERS), 0], g_recv.at[i, k])

    def new_rows(k, l, s, scale, take):
        start = pl.multiple_of((2 * chip_of(s) + core) * dims[k][0], dims[k][0])

        def run(i, carry):
            at = i * 16
            replicas[k][l, pl.ds(pl.multiple_of(start + at, 16), 16), :] = take(pl.ds(pl.multiple_of(at, 16), 16), scale).astype(jnp.bfloat16)
            return carry

        lax.fori_loop(0, dims[k][0] // 16, run, 0)

    for g, kinds in enumerate(NORM_GROUPS):
        roots = jnp.sqrt(shared(g))
        scales = {(k, l): LEARN_RATE * (pick(roots, 2 * k + l) / pick(roots, 8 + 2 * k + l)) for k in kinds for l in range(LAYERS)}
        if g == 0:
            await_bytes(early_w, early_sem.at[0])
        for k in kinds:
            for l in range(LAYERS):

                def fresh_rows(r, scale):
                    fresh = wv[k][l, r, :] - scale * acc[k][l, ME, r, :]
                    wv[k][l, r, :] = fresh
                    return fresh

                new_rows(k, l, ME, scales[k, l], fresh_rows)
                own_copy(l, 1 if g == 0 else 0, k).start()
        if g == 0:
            first_scales = scales
            for l in range(LAYERS):
                half_copy(l, ME, first_kind).start()

    for k in later_kinds:
        for l in range(LAYERS):
            own_copy(l, 1, k).start()
            half_copy(l, ME, k).start()

    await_bytes(early_w, early_sem.at[1])
    await_bytes(early_u, early_sem.at[3])
    for l in range(LAYERS):
        new_rows(first_kind, l, first_nb[l], first_scales[first_kind, l], lambda r, scale: early_w[l, r, :] - scale * early_u[l, r, :])
        half_copy(l, first_nb[l], first_kind).start()
    for k in later_kinds:
        await_blocks(0, k)
        for l in range(LAYERS):
            if k != later_kinds[0]:
                pass_copy(l, k).start()
            half_copy(l, first_nb[l], k).start()
    for l in range(LAYERS):
        pass_copy(l, later_kinds[0]).start()
    half = dims[first_kind][0] // 2

    def part_block(l, s, upper):
        start = pl.multiple_of((2 * chip_of(s) + core) * dims[first_kind][0] + upper * half, half)
        return replicas[first_kind].at[l, pl.ds(start, half)]

    def last_copy(l, other_core):
        src = part_block(l, first_nb[l], 1)
        send = h_send if other_core else g_send
        return remote(src, src, send.at[first_kind], tail_sem.at[other_core], device(second_nb[l], bool(other_core)))

    for l in range(LAYERS):
        src = part_block(l, first_nb[l], 0)
        remote(src, src, g_send.at[first_kind], g_recv.at[2, first_kind], second_dev[l]).start()
    for l in range(LAYERS):
        for other_core in range(2):
            last_copy(l, other_core).start()
    for k in KIND_ORDER:
        await_blocks(1, k)
        for l in range(LAYERS):
            half_copy(l, second_nb[l], k).start()
    for k in later_kinds[1:] + later_kinds[:1]:
        await_blocks(2, k)
        for l in range(LAYERS):
            half_copy(l, DG, k).start()
    half_bytes = got[first_kind].at[pl.ds(0, LAYERS), 0, pl.ds(0, half)]
    await_bytes(half_bytes, g_recv.at[2, first_kind])
    for l in range(LAYERS):
        src = part_block(l, DG, 0)
        remote(src, src, h_send.at[first_kind], h_recv.at[first_kind], partner).start()
    for other_core in range(2):
        await_bytes(half_bytes, tail_sem.at[other_core])

    for k in range(KINDS):
        if k == first_kind:
            await_bytes(sent[k].at[pl.ds(0, LAYERS), pl.ds(0, 3)], d_send.at[k])
            await_bytes(p1[k].at[pl.ds(0, LAYERS), 1], p1_send.at[k])
        else:
            await_bytes(sent[k], d_send.at[k])
            await_bytes(p1[k], p1_send.at[k])
        await_bytes(p2[k], p2_send.at[k])
        await_bytes(got[k].at[pl.ds(0, LAYERS), pl.ds(0, 2 if k == first_kind else 3)], g_send.at[k])
        await_bytes(got[k], h_send.at[k])
        if k == first_kind:
            await_bytes(replicas[2].at[0, pl.ds(0, LAYERS * 7 * half)], h_recv.at[k])
        else:
            await_bytes(got[k], h_recv.at[k])
    await_bytes(raw_in, raw_sem.at[0])
    await_bytes(raw_peer, raw_sem.at[2])
    await_bytes(early_u, early_sem.at[2])
    await_bytes(all_ref.at[pl.ds(0, GROUPS + 1), pl.ds(0, n_dev - 1)], ps_send.at[0])


def write_out(count, *refs):
    srcs, dsts, sems = refs[:count], refs[count:2 * count], refs[2 * count]
    pieces = 4
    for i, (src, dst) in enumerate(zip(srcs, dsts)):
        rows = src.shape[1] // pieces
        for l in range(LAYERS):
            for h in range(pieces):
                part = (l, pl.ds(h * rows, rows))
                pltpu.make_async_copy(src.at[part], dst.at[part], sems.at[i]).start()
    for i, (src, dst) in enumerate(zip(srcs, dsts)):
        pltpu.make_async_copy(src, dst, sems.at[i]).wait()


def solution(mesh):
    n_model, n_data = mesh.shape["model"], mesh.shape["data"]
    in_specs = []
    for col_split in COLUMN_SPLIT:
        in_specs.extend([grad_spec(col_split), state_spec(col_split), state_spec(col_split), state_spec(col_split)])
    out_specs = tuple([replica_spec(col_split) for col_split in COLUMN_SPLIT] + [state_spec(col_split) for col_split in COLUMN_SPLIT] * 3)

    def device_step(*arrays):
        dims = [arrays[4 * k + 1].shape[1:] for k in range(KINDS)]
        f32, bf16 = jnp.float32, jnp.bfloat16
        out_shape = [jax.ShapeDtypeStruct((LAYERS, n_data * d[0], d[1]), bf16) for d in dims]
        out_shape += [jax.ShapeDtypeStruct((LAYERS,) + tuple(d), f32) for d in dims] * 3

        def each(prefix, dtype):
            return [pltpu.VMEM(prefix + tuple(d), dtype) for d in dims]

        dma = pltpu.SemaphoreType.DMA
        n_dev = n_model * n_data
        scratch = (each((LAYERS, 4), f32) + each((LAYERS,), f32) + each((LAYERS, 4), bf16) + each((LAYERS, 4), bf16)
                   + each((LAYERS, 2), f32) + each((LAYERS,), f32))
        scratch += [pltpu.VMEM((GROUPS + 1, 1, 128), f32), pltpu.VMEM((GROUPS + 1, n_dev, 1, 128), f32)]
        scratch += [dma((4, 2)), dma((4,)), dma((4,)), dma((4, 4)), dma((4,)), dma((2, 4)), dma((4,)), dma((4,)),
                    dma((4,)), dma((3, 4)), dma((4,)), dma((4,)), dma((1,)), dma((GROUPS + 1,)), dma((4,)), dma((4,)), dma((2,)), pltpu.SemaphoreType.REGULAR((n_model + 1,))]
        first = tuple(dims[KIND_ORDER[0]])
        scratch += [pltpu.VMEM((LAYERS, 2) + first, bf16), pltpu.VMEM((LAYERS, 2) + first, bf16), pltpu.VMEM((LAYERS,) + first, bf16)]
        scratch += [pltpu.VMEM((LAYERS,) + first, f32)] * 2
        held = pl.pallas_call(
            functools.partial(kernel, n_model, n_data, dims),
            out_shape=[pltpu.VMEM(o.shape, o.dtype) for o in out_shape],
            in_specs=[pl.BlockSpec(memory_space=pl.ANY)] * 16,
            out_specs=[pl.BlockSpec(memory_space=pltpu.VMEM)] * 16,
            scratch_shapes=scratch,
            compiler_params=pltpu.CompilerParams(collective_id=0, has_side_effects=True, vmem_limit_bytes=COMM_VMEM),
            name="lamb_step",
        )(*arrays)
        held = [pltpu.with_memory_space_constraint(h, pltpu.VMEM) for h in held]
        return tuple(pl.pallas_call(
            functools.partial(write_out, len(out_shape)),
            out_shape=out_shape,
            in_specs=[pl.BlockSpec(memory_space=pltpu.VMEM)] * 16,
            out_specs=[pl.BlockSpec(memory_space=pl.ANY)] * 16,
            scratch_shapes=[dma((16,))],
            compiler_params=pltpu.CompilerParams(vmem_limit_bytes=1 << 20),
            name="write_out",
        )(*held))

    return jax.shard_map(device_step, mesh=mesh, in_specs=tuple(in_specs), out_specs=out_specs, check_vma=False)
```
